256 devices in a mesh: row: 16 (over x, y), col: 16 (over z, core).
Axes of the slice: x: 4, y: 4, z: 8, core: 2. Of those that a mesh axis runs over, the one named last changes fastest.
Arguments:
- head_start: float32 [6144, 16384], P('row', 'col'), may hold values from -6 to 6
- recharge: float32 [6144, 16384], P('row', 'col'), may hold values from -4 to 4
- storage: float32 [6144, 16384], P('row', 'col'), may hold values from 0.02 to 0.5
- seg_block: int32 [262144], P(('row', 'col')), may hold values from 0 to 3071
- seg_mask: int32 [262144, 128], P(('row', 'col')), may hold values 0 or 1
- seg_cond: float32 [262144, 128], P(('row', 'col')), may hold values from 0.02 to 0.2
- seg_reach: int32 [262144], P(('row', 'col')), may hold values from 0 to 65535, as said below
- reach_bed: float32 [65536], P(('row', 'col')), may hold values from -1 to 1
- section_start: float32 [65536], P(('row', 'col')), may hold values from 0 to 2
- reach_net: int32 [65536], P(('row', 'col')), may hold values from 0 to 63
- net_inflow: float32 [64], replicated, may hold values from 2 to 16
Outputs:
- head: float32 [6144, 16384], P('row', 'col')
- section: float32 [65536], P(('row', 'col'))
The draws below stay inside these ranges and needn't reach their ends.
Inputs may be any that keep to these rules, and one draw needn't show every extreme that they name: `seg_reach`: A segment on device (i, j) names a reach owned by device (i, j - 1), (i, j) or (i, j + 1), columns taken modulo 16, where reach r is owned by device r // 256 in the numbering i * 16 + j.
All inputs are finite; a program needn't handle non-finite values. No bound on the sum of `seg_mask` on one device may be relied on, other than what follows from the above.
Results may differ from the reference program's by a relative error of at most 0.00029.
Values sent between devices are 32-bit elements; how exact they have to be, the bound alone decides.
No kernel may reach another device: no remote copies, remote signals or barrier semaphores. Data moves between devices by JAX's collectives and lax.ppermute only.
A program may use at most 64 MiB of HBM per device.

```python
import math
import jax
import jax.numpy as jnp
from jax import lax

CR = 384
CC = 1024
SEG_DEV = 1024
REACH_DEV = 256
NETS = 64
PICARD = 2
SWEEPS = 4
NR = 6144
NC = 16384
BLK = 3072
SEGS = 262144
R = 65536
N_ROW = 16
N_COL = 16


def draw_seg_reach(key, part):
    first, second = jax.random.split(jax.random.fold_in(key, 11))
    slots = jnp.arange(SEGS, dtype=jnp.int32)
    device = slots // SEG_DEV
    row_pos = device // N_COL
    col_pos = device % N_COL
    offset = jax.random.randint(first, slots.shape, -1, 2, dtype=jnp.int32)
    owner_col = (col_pos + offset + N_COL) % N_COL
    inner = jax.random.randint(second, slots.shape, 0, REACH_DEV, dtype=jnp.int32)
    return ((row_pos * N_COL + owner_col) * REACH_DEV + inner).astype(jnp.int32)


def touch_ends(entries, rng, low, high):
    shape = entries.shape
    place = [jax.random.randint(jax.random.fold_in(rng, axis), (), 0, shape[axis]) for axis in range(len(shape))]
    entries = entries.at[tuple(place)].set(low)
    longest = shape.index(max(shape))
    place[longest] = (place[longest] + 1) % shape[longest]
    return entries.at[tuple(place)].set(high)


def shard_levels(key, shape, shards, smallest, high):
    factor_of = 1.0
    for axis_at, parts in shards:
        heights = jax.random.uniform(jax.random.fold_in(jax.random.fold_in(key, 6), axis_at), (parts,), jnp.float32, smallest / len(shards), high / len(shards))
        factor_of = factor_of * jnp.repeat(jnp.exp(heights), shape[axis_at] // parts).reshape((-1,) + (1,) * (len(shape) - 1 - axis_at))
    return factor_of


def centred(rng, extent, width, bound, pieces=(), held_as=jnp.bfloat16):
    loudness = shard_levels(rng, extent, pieces, -0.22, 0.18) if pieces else 1.0
    result = jax.random.normal(rng, extent, jnp.float32) * width * loudness
    return jnp.minimum(jnp.maximum(result, -bound), bound).astype(held_as)


def setup_inputs(seed: int = 0) -> dict:
    seeds = jax.random.split(jax.random.key(seed), 12)
    return {
        "head_start": centred(seeds[0], (NR, NC), 1.0, 6.0, ((0, 16), (1, 16)), jnp.float32),
        "recharge": centred(seeds[1], (NR, NC), 0.5, 4.0, ((0, 16), (1, 16)), jnp.float32),
        "storage": jnp.clip(jnp.exp(math.log(0.5) - 3.218876 * jax.random.uniform(seeds[2], (NR, NC), jnp.float32) ** shard_levels(seeds[2], (NR, NC), ((0, 16), (1, 16)), -0.2, 0.2)), 0.02, 0.5),
        "seg_block": touch_ends(jax.random.randint(seeds[3], (SEGS,), 0, BLK), jax.random.fold_in(seeds[3], 1), 0, BLK - 1).astype(jnp.int32),
        "seg_mask": touch_ends((jax.random.randint(seeds[4], (SEGS, 128), 0, 4) < 1).astype(jnp.int32), jax.random.fold_in(seeds[4], 1), 0, 1),
        "seg_cond": jnp.clip(jnp.exp(math.log(0.2) - 2.3025851 * jax.random.uniform(seeds[5], (SEGS, 128), jnp.float32) ** shard_levels(seeds[5], (SEGS, 128), ((0, 256),), -0.2, 0.2)), 0.02, 0.2),
        "seg_reach": draw_seg_reach(jax.random.fold_in(seeds[11], 71), 0),
        "reach_bed": jnp.clip(jax.random.uniform(seeds[7], (R,), jnp.float32, -1.0, 1.0) * shard_levels(seeds[7], (R,), ((0, 256),), -0.4, 0.0), -1.0, 1.0),
        "section_start": jnp.clip(2.0 * jax.random.uniform(seeds[8], (R,), jnp.float32) ** shard_levels(seeds[8], (R,), ((0, 256),), -0.2, 0.2), 0.0, 2.0),
        "reach_net": touch_ends(jax.random.randint(seeds[9], (R,), 0, NETS), jax.random.fold_in(seeds[9], 1), 0, NETS - 1).astype(jnp.int32),
        "net_inflow": jnp.clip(jnp.exp(jax.random.uniform(seeds[10], (NETS,), jnp.float32, math.log(2.0), math.log(16.0))), 2.0, 16.0),
    }


def relax(padded, storage, supply, cond, source):
    beside = padded[:-2, 1:-1] + padded[2:, 1:-1] + padded[1:-1, :-2] + padded[1:-1, 2:]
    return (beside + supply + source) / (4.0 + storage + cond)

def reference(head_start, recharge, storage, seg_block, seg_mask, seg_cond, seg_reach, reach_bed, section_start, reach_net, net_inflow):
    devices = N_ROW * N_COL
    blocks = CR * CC // 128

    def to_blocks(grid):
        return grid.reshape(N_ROW, CR, N_COL, CC).transpose(0, 2, 1, 3).reshape(devices * blocks, 128)

    def from_blocks(table):
        return table.reshape(N_ROW, N_COL, CR, CC).transpose(0, 2, 1, 3).reshape(N_ROW * CR, N_COL * CC)
    row_ids = (jnp.arange(SEGS, dtype=jnp.int32) // SEG_DEV * blocks + seg_block).astype(jnp.int32)
    weight = seg_mask.astype(jnp.float32) * seg_cond
    cond = from_blocks(jax.ops.segment_sum(weight, row_ids, devices * blocks))
    inflow = net_inflow[reach_net]
    supply = storage * head_start + recharge
    head = head_start
    section = section_start
    section_seg = section[seg_reach]
    for step in range(PICARD):
        head_seg = to_blocks(head)[row_ids]
        leak = lax.optimization_barrier(jnp.sum(weight * (section_seg[:, None] - head_seg), axis=1))
        total = jax.ops.segment_sum(leak, seg_reach, R)
        section = reach_bed + jnp.sqrt(1.0 + jax.nn.softplus(inflow - total)) - 1.0
        section_seg = section[seg_reach]
        source = from_blocks(jax.ops.segment_sum(weight * section_seg[:, None], row_ids, devices * blocks))
        for sweep in range(SWEEPS):
            head = relax(jnp.pad(head, 1), storage, supply, cond, source)
    return (head, section)
```

```python
import functools

import jax
import jax.numpy as jnp
from jax import lax
from jax.experimental import pallas as pl
from jax.experimental.pallas import tpu as pltpu
from jax.sharding import PartitionSpec as P

NETS = 64
SWEEPS = 4
ROWS, COLS = 384, 1024
TILES = COLS // 128
SEG = 1024
REACH = 256
FRAME = 4 * REACH
OFF = 16
EXT = ROWS + 2 * OFF
H = 4
CHUNKS = ROWS // 8 + 2
F32 = jnp.float32
BF16 = jnp.bfloat16


def spec(space=pltpu.VMEM):
    return pl.BlockSpec(memory_space=space)


def split2(x):
    hi = x.astype(BF16)
    lo = (x - hi.astype(F32)).astype(BF16)
    return hi, lo


def column_of(row):
    return jnp.broadcast_to(row, (128, 128)).T


def gather_rows(read, blk, out):
    def group(g, carry):
        for u in range(16):
            s = g * 16 + u
            b = blk[s]
            out[pl.ds(s, 1), :] = read(b >> 3, b & 7)
        return carry

    lax.fori_loop(0, SEG // 16, group, 0)


def row_sums(get, lhs, first):
    for k in range(SEG // 128):
        at = slice(k * 128, (k + 1) * 128)
        row = jnp.sum(get(at).T, axis=0, keepdims=True)
        hi = row.astype(BF16).astype(F32)
        mid = (row - hi).astype(BF16).astype(F32)
        lhs[first : first + 1, at] = hi
        lhs[first + 1 : first + 2, at] = mid
        lhs[first + 2 : first + 3, at] = row - hi - mid


def clear_rim(ref):
    zero = jnp.zeros((OFF, 128), F32)
    for c in range(TILES):
        ref[c, 0:OFF, :] = zero
        ref[c, OFF + ROWS : EXT, :] = zero
    ref[TILES, :, :] = jnp.zeros((EXT, 128), F32)


def prep(head, blk, reach, mask, condu, bed, sec0, net, infl, part, oh, weight, headx, hs, lhs):
    j = lax.axis_index("col")
    base = (j // 2) * 2 - 1
    reach8 = reach[...]
    slot8 = (((reach8 // REACH) % 16 - base + 16) % 16) * REACH + reach8 % REACH

    def read(r, c):
        return headx[c, pl.ds(r + OFF, 1), :]

    clear_rim(headx)
    for c in range(TILES):
        headx[c, OFF : OFF + ROWS, :] = head[:, c * 128 : (c + 1) * 128]
    weight[...] = mask[...].astype(F32) * condu[...]
    gather_rows(read, blk, hs)
    lhs[...] = jnp.zeros_like(lhs)
    row_sums(lambda at: weight[at, :] * hs[at, :], lhs, 0)
    row_sums(lambda at: weight[at, :], lhs, 3)
    lane = lax.broadcasted_iota(jnp.int32, (128, 128), 1)
    for k in range(SEG // 128):
        slots = column_of(slot8[k : k + 1, :])
        for q in range(FRAME // 128):
            oh[k * 128 : (k + 1) * 128, q * 128 : (q + 1) * 128] = jnp.where(
                slots == lane + q * 128, 1.0, 0.0
            ).astype(BF16)
    sums = jnp.dot(lhs[...].astype(BF16), oh[...], preferred_element_type=F32)
    part[...] = jnp.zeros_like(part)
    part[0:1, :] = sums[0:1] + sums[1:2] + sums[2:3]
    part[1:2, :] = sums[3:4] + sums[4:5] + sums[5:6]
    nets = net[...]
    inflow = jnp.zeros(nets.shape, F32)
    for n in range(NETS):
        inflow = jnp.where(nets == n, infl[n], inflow)
    values = (bed[...], inflow, sec0[...])
    odd = j % 2
    for w in range(2):
        keep = odd == w
        for t in range(2):
            at = (1 + w) * REACH + t * 128
            for q, v in enumerate(values):
                part[2 + q : 3 + q, at : at + 128] = jnp.where(keep, v[t : t + 1, :], 0.0)


def fields(headx, recharge, storage, blk8, weight, onehot, inv, supply):
    blk = blk8[...]
    target = (blk & 7) * ROWS + (blk >> 3)
    iota = lax.broadcasted_iota(jnp.int32, (ROWS, 128), 0)
    for k in range(SEG // 128):
        row = jnp.broadcast_to(target[k : k + 1, :], (ROWS, 128))
        for c in range(TILES):
            onehot[c * ROWS : (c + 1) * ROWS, k * 128 : (k + 1) * 128] = jnp.where(
                row == iota + c * ROWS, 1.0, 0.0
            ).astype(BF16)
    hi, lo = split2(weight[...])
    both = jnp.concatenate([hi, lo], axis=1)
    clear_rim(inv)
    for c in range(TILES):
        at = slice(c * 128, (c + 1) * 128)
        got = jnp.dot(onehot[c * ROWS : (c + 1) * ROWS, :], both, preferred_element_type=F32)
        cond = got[:, :128] + got[:, 128:]
        start = headx[c, OFF : OFF + ROWS, :]
        store = storage[:, at]
        inv[c, OFF : OFF + ROWS, :] = 1.0 / (4.0 + store + cond)
        supply[c] = store * start + recharge[:, at]


def source_kernel(first, *refs):
    if first:
        own, up, down, oh, onehot, weight, supply, inv, headx, frame, section, rhs, sa, sb = refs
        fields_sent = (headx, rhs, inv)
    else:
        own, up, down, old, oh, onehot, weight, supply, headx, section, rhs, sa, sb = refs
        fields_sent = (headx, rhs)
    i = lax.axis_index("row")
    j = lax.axis_index("col")
    full = own[...] + jnp.concatenate([up[...], down[...]], axis=1)
    leak = full[0:1]
    if first:
        wsum, bed, inflow, sec = full[1:2], full[2:3], full[3:4], full[4:5]
    else:
        wsum, bed, inflow, sec = (old[q : q + 1, :] for q in (1, 2, 3, 4))
    x = inflow - (sec * wsum - leak)
    soft = jnp.maximum(x, 0.0) + jnp.log1p(jnp.exp(-jnp.abs(x)))
    sec = bed + jnp.sqrt(1.0 + soft) - 1.0
    if first:
        frame[...] = full
        frame[4:5, :] = sec
    odd = j % 2 == 1
    for t in range(2):
        a = REACH + t * 128
        b = 2 * REACH + t * 128
        section[t : t + 1, :] = jnp.where(odd, sec[:, b : b + 128], sec[:, a : a + 128])
    hi, lo = split2(sec)
    wide = jnp.concatenate(
        [jnp.broadcast_to(hi.astype(F32), (128, FRAME)), jnp.broadcast_to(lo.astype(F32), (128, FRAME))], axis=0
    ).astype(BF16)
    got = lax.dot_general(oh[...], wide, (((1,), (1,)), ((), ())), preferred_element_type=F32)
    hi, lo = split2(weight[...] * (got[:, :128] + got[:, 128:]))
    both = jnp.concatenate([hi, lo], axis=1)
    clear_rim(rhs)
    for c in range(TILES):
        got = jnp.dot(onehot[c * ROWS : (c + 1) * ROWS, :], both, preferred_element_type=F32)
        rhs[c, OFF : OFF + ROWS, :] = supply[c] + got[:, :128] + got[:, 128:]
    row_odd = i % 2 == 1
    if sa.shape[1] > len(fields_sent) * H:
        sa[...] = jnp.zeros_like(sa)
        sb[...] = jnp.zeros_like(sb)
    for q, ref in enumerate(fields_sent):
        top = ref[0:TILES, OFF : OFF + H, :]
        bottom = ref[0:TILES, OFF + ROWS - H : OFF + ROWS, :]
        sa[:, q * H : (q + 1) * H, :] = jnp.where(row_odd, top, bottom)
        sb[:, q * H : (q + 1) * H, :] = jnp.where(row_odd, bottom, top)


def columns(*refs):
    count = (len(refs) - 2)
    ma, mb = refs[count:]
    odd = lax.axis_index("col") % 2 == 1
    ma[...] = jnp.zeros_like(ma)
    mb[...] = jnp.zeros_like(mb)
    for q in range(count):
        for k in range(ROWS // 128):
            at = slice(OFF + k * 128, OFF + (k + 1) * 128)
            left = refs[q][0, at, :].T[0:H, :]
            right = refs[q][TILES - 1, at, :].T[128 - H : 128, :]
            ma[q * H : (q + 1) * H, k * 128 : (k + 1) * 128] = jnp.where(odd, left, right)
            mb[q * H : (q + 1) * H, k * 128 : (k + 1) * 128] = jnp.where(odd, right, left)


def top_bottom(ra, rb):
    i = lax.axis_index("row")
    odd = i % 2 == 1
    top = jnp.where(i == 0, 0.0, jnp.where(odd, ra, rb))
    bottom = jnp.where(i == 15, 0.0, jnp.where(odd, rb, ra))
    return top, bottom


def corners(ra, rb, ma, mb, na, nb, tall):
    odd = lax.axis_index("col") % 2 == 1
    depth = ra.shape[1]
    parts = []
    for c in (0, TILES - 1):
        top, bottom = top_bottom(ra[c], rb[c])
        tall[...] = jnp.zeros_like(tall)
        tall[0:depth, :] = top
        tall[depth : 2 * depth, :] = bottom
        turned = tall[...].T
        parts.append(turned[0:H, :] if c == 0 else turned[128 - H : 128, :])
    left, right = parts
    na[...] = ma[...]
    nb[...] = mb[...]
    na[0:H, ROWS : ROWS + 128] = jnp.where(odd, left, right)
    nb[0:H, ROWS : ROWS + 128] = jnp.where(odd, right, left)


def sweep(src, dst, rhs, inv):
    lane = lax.broadcasted_iota(jnp.int32, (8, 128), 1)
    first = lane == 0
    last = lane == 127

    def chunk(k):
        r = 8 + k * 8
        mid = [src[c, pl.ds(r, 8), :] for c in range(TILES + 1)]
        fwd = [pltpu.roll(m, 1, 1) for m in mid]
        bwd = [pltpu.roll(m, 127, 1) for m in mid]
        for c in range(TILES + 1):
            left = jnp.where(first, fwd[c - 1], fwd[c])
            right = jnp.where(last, bwd[(c + 1) % (TILES + 1)], bwd[c])
            beside = src[c, pl.ds(r - 1, 8), :] + src[c, pl.ds(r + 1, 8), :]
            total = beside + (left + right) + rhs[c, pl.ds(r, 8), :]
            dst[c, pl.ds(r, 8), :] = total * inv[c, pl.ds(r, 8), :]

    def group(g, carry):
        for u in range(5):
            chunk(g * 5 + u)
        return carry

    lax.fori_loop(0, CHUNKS // 5, group, 0)


def place_halo(refs, ra, rb, ca, cb, wide):
    depth = ra.shape[1]
    j = lax.axis_index("col")
    odd = j % 2 == 1
    top, bottom = top_bottom(ra[...], rb[...])
    right = jnp.where(j == 15, 0.0, jnp.where(odd, cb[...], ca[...]))
    left = jnp.where(j == 0, 0.0, jnp.where(odd, ca[...], cb[...]))
    wide[...] = jnp.zeros_like(wide)
    wide[0:H, 0:128] = right[0:H, ROWS : ROWS + 128]
    wide[128 - H : 128, 0:128] = left[0:H, ROWS : ROWS + 128]
    turned = wide[:, 0:128].T
    for q, ref in enumerate(refs):
        own = slice(q * H, (q + 1) * H)
        ref[0:TILES, OFF - H : OFF, :] = top[:, own, :]
        ref[0:TILES, OFF + ROWS : OFF + ROWS + H, :] = bottom[:, own, :]
        ref[TILES, OFF - H : OFF, :] = turned[own, :]
        ref[TILES, OFF + ROWS : OFF + ROWS + H, :] = turned[depth + q * H : depth + (q + 1) * H, :]
        wide[0:H, :] = right[own, 0:ROWS]
        wide[128 - H : 128, :] = left[own, 0:ROWS]
        for k in range(ROWS // 128):
            ref[TILES, OFF + k * 128 : OFF + (k + 1) * 128, :] = wide[:, k * 128 : (k + 1) * 128].T


def relax_first(ra, rb, ca, cb, head_in, rhs_in, inv_in, blk, weight, oh, head, rhs, inv, part, other, wide, hs, lhs):
    place_halo((head, rhs, inv), ra, rb, ca, cb, wide)
    for c in range(TILES + 1):
        other[c, 0:8, :] = jnp.zeros((8, 128), F32)
        other[c, EXT - 8 : EXT, :] = jnp.zeros((8, 128), F32)
    for _ in range(SWEEPS // 2):
        sweep(head, other, rhs, inv)
        sweep(other, head, rhs, inv)

    def read(r, c):
        return head[c, pl.ds(r + OFF, 1), :]

    gather_rows(read, blk, hs)
    lhs[...] = jnp.zeros_like(lhs)
    row_sums(lambda at: weight[at, :] * hs[at, :], lhs, 0)
    sums = jnp.dot(lhs[...].astype(BF16), oh[...], preferred_element_type=F32)
    part[...] = jnp.zeros_like(part)
    part[0:1, :] = sums[0:1] + sums[1:2] + sums[2:3]


def relax_last(ra, rb, ca, cb, head_in, rhs_in, inv, out, head, rhs, other, wide):
    place_halo((head, rhs), ra, rb, ca, cb, wide)
    for c in range(TILES + 1):
        other[c, 0:8, :] = jnp.zeros((8, 128), F32)
        other[c, EXT - 8 : EXT, :] = jnp.zeros((8, 128), F32)
    for _ in range(SWEEPS // 2):
        sweep(head, other, rhs, inv)
        sweep(other, head, rhs, inv)
    for c in range(TILES):
        out[:, c * 128 : (c + 1) * 128] = head[c, OFF : OFF + ROWS, :]


def shape(*dims, dtype=F32):
    return jax.ShapeDtypeStruct(dims, dtype)


def call(kernel, outs, ins, name, scratch=(), smem=(), aliases=None, limit=20, flops=10_000_000):
    return pl.pallas_call(
        kernel,
        out_shape=outs,
        in_specs=[spec(pltpu.SMEM) if k in smem else spec() for k in range(len(ins))],
        out_specs=jax.tree.map(lambda _: spec(), outs),
        scratch_shapes=list(scratch),
        input_output_aliases=aliases or {},
        compiler_params=pltpu.CompilerParams(vmem_limit_bytes=limit * 2**20),
        cost_estimate=pl.CostEstimate(flops=flops, bytes_accessed=4_000_000, transcendentals=0),
        name=name,
    )(*ins)


def swap(x, axis, which):
    n = lax.axis_size(axis)
    if which == 0:
        pairs = [(k, k ^ 1) for k in range(n)]
    else:
        pairs = [(k, (k + 1) % n if k % 2 else (k - 1) % n) for k in range(n)]
    return lax.ppermute(x, axis, pairs)


def shift(x, axis, by):
    n = lax.axis_size(axis)
    return lax.ppermute(x, axis, [(k, (k + by) % n) for k in range(n)])


def exchange_sums(part):
    both = part + swap(part, "col", 0)
    up = shift(both[:, 2 * REACH :], "col", 2)
    down = shift(both[:, : 2 * REACH], "col", -2)
    return both, up, down


ext = shape(TILES + 1, EXT, 128)


def halo_exchange(sent, sa, sb, count):
    depth = 16 if count == 3 else 8
    ma, mb = call(columns, (shape(depth, 512), shape(depth, 512)), sent, "cols")
    ra = swap(sa, "row", 0)
    rb = swap(sb, "row", 1)
    na, nb = call(
        corners,
        (shape(depth, 512), shape(depth, 512)),
        (ra, rb, ma, mb),
        "corners",
        scratch=[pltpu.VMEM((128, 128), F32)],
    )
    ca = swap(na, "col", 0)
    cb = swap(nb, "col", 1)
    return ra, rb, ca, cb


def body(head0, recharge, storage, seg_block, seg_mask, seg_cond, seg_reach, bed, sec0, net, infl):
    blk8 = seg_block.reshape(8, 128)
    part, oh, weight, headx = call(
        prep,
        (shape(8, FRAME), shape(SEG, FRAME, dtype=BF16), shape(SEG, 128), ext),
        (
            head0,
            seg_block,
            seg_reach.reshape(8, 128),
            seg_mask,
            seg_cond,
            bed.reshape(2, 128),
            sec0.reshape(2, 128),
            net.reshape(2, 128),
            infl,
        ),
        "prep",
        scratch=[pltpu.VMEM((SEG, 128), F32), pltpu.VMEM((16, SEG), F32)],
        smem=(1, 8),
    )
    both, up, down = exchange_sums(part)
    onehot, inv, supply = call(
        fields,
        (shape(TILES * ROWS, SEG, dtype=BF16), ext, shape(TILES, ROWS, 128)),
        (headx, recharge, storage, blk8, weight),
        "fields",
        limit=24,
    )
    strip = shape(TILES, 16, 128)
    frame, section, rhs, sa, sb = call(
        functools.partial(source_kernel, True),
        (shape(8, FRAME), shape(2, 128), ext, strip, strip),
        (both, up, down, oh, onehot, weight, supply, inv, headx),
        "source1",
        limit=24,
    )
    ra, rb, ca, cb = halo_exchange((headx, rhs, inv), sa, sb, 3)
    head, rhs, inv, part = call(
        relax_first,
        (ext, ext, ext, shape(8, FRAME)),
        (ra, rb, ca, cb, headx, rhs, inv, seg_block, weight, oh),
        "relax1",
        scratch=[
            pltpu.VMEM((TILES + 1, EXT, 128), F32),
            pltpu.VMEM((128, ROWS), F32),
            pltpu.VMEM((SEG, 128), F32),
            pltpu.VMEM((16, SEG), F32),
        ],
        smem=(7,),
        aliases={4: 0, 5: 1, 6: 2},
    )
    both, up, down = exchange_sums(part)
    strip = shape(TILES, 8, 128)
    section, rhs, sa, sb = call(
        functools.partial(source_kernel, False),
        (shape(2, 128), ext, strip, strip),
        (both, up, down, frame, oh, onehot, weight, supply, head),
        "source2",
        limit=24,
    )
    ra, rb, ca, cb = halo_exchange((head, rhs), sa, sb, 2)
    out, head, rhs = call(
        relax_last,
        (shape(ROWS, COLS), ext, ext),
        (ra, rb, ca, cb, head, rhs, inv),
        "relax2",
        scratch=[pltpu.VMEM((TILES + 1, EXT, 128), F32), pltpu.VMEM((128, ROWS), F32)],
        aliases={4: 1, 5: 2},
    )
    return out, section.reshape(REACH)


def solution(mesh):
    placed = (
        P("row", "col"),
        P("row", "col"),
        P("row", "col"),
        P(("row", "col")),
        P(("row", "col"), None),
        P(("row", "col"), None),
        P(("row", "col")),
        P(("row", "col")),
        P(("row", "col")),
        P(("row", "col")),
        P(),
    )
    return jax.shard_map(
        body,
        mesh=mesh,
        in_specs=placed,
        out_specs=(P("row", "col"), P(("row", "col"))),
        check_vma=False,
    )
```

```python
import functools

import jax
import jax.numpy as jnp
from jax import lax
from jax.experimental import pallas as pl
from jax.experimental.pallas import tpu as pltpu
from jax.sharding import PartitionSpec as P

NETS = 64
SWEEPS = 4
ROWS, COLS = 384, 1024
TILES = COLS // 128
WIDE = TILES + 1
SEG = 1024
REACH = 256
FRAME = 4 * REACH
OFF = 8
EXT = ROWS + 2 * OFF
H = 4
DEPTH = (4, 3, 3)
UNROLL = 12
F32 = jnp.float32
BF16 = jnp.bfloat16
I32 = jnp.int32


def split2(x):
    hi = x.astype(BF16)
    lo = (x - hi.astype(F32)).astype(BF16)
    return hi, lo


def both_halves(x):
    return jnp.concatenate(split2(x), axis=1)


def column_of(row):
    return jnp.broadcast_to(row, (128, 128)).T


def tile_rows(c, start, size):
    return slice(c * EXT + OFF + start, c * EXT + OFF + start + size)


def gather_rows(head, index, out):
    def group(k, carry):
        for u in range(128):
            out[pl.ds(k * 128 + u, 1), :] = head[pl.ds(index[k, u], 1), :]
        return carry

    lax.fori_loop(0, SEG // 128, group, 0)


def row_sums(get, lhs, first):
    for k in range(SEG // 128):
        at = slice(k * 128, (k + 1) * 128)
        row = jnp.sum(get(at).T, axis=0, keepdims=True)
        hi = row.astype(BF16).astype(F32)
        mid = (row - hi).astype(BF16).astype(F32)
        lhs[first : first + 1, at] = hi
        lhs[first + 1 : first + 2, at] = mid
        lhs[first + 2 : first + 3, at] = row - hi - mid


def prep(
    head, blk, reach, mask, condu, bed, sec0, net, infl,
    part, oh, weight, headx, index8,
    hs, lhs, blk_v, reach_v, mask_v, cond_v, bed_v, sec0_v, net_v, infl_s, index_s, sems,
):
    moves = [
        pltpu.make_async_copy(blk, blk_v, sems.at[0]),
        pltpu.make_async_copy(reach, reach_v, sems.at[1]),
        pltpu.make_async_copy(mask, mask_v, sems.at[2]),
        pltpu.make_async_copy(condu, cond_v, sems.at[3]),
        pltpu.make_async_copy(bed, bed_v, sems.at[4]),
        pltpu.make_async_copy(sec0, sec0_v, sems.at[5]),
        pltpu.make_async_copy(net, net_v, sems.at[6]),
        pltpu.make_async_copy(infl, infl_s, sems.at[7]),
    ]
    heads = [
        pltpu.make_async_copy(
            head.at[:, c * 128 : (c + 1) * 128], headx.at[tile_rows(c, 0, ROWS), :], sems.at[8 + c]
        )
        for c in range(TILES)
    ]
    for m in moves + heads:
        m.start()
    j = lax.axis_index("col")
    base = (j // 2) * 2 - 1
    for c in range(WIDE):
        headx[c * EXT : c * EXT + OFF, :] = jnp.zeros((OFF, 128), F32)
        headx[(c + 1) * EXT - OFF : (c + 1) * EXT, :] = jnp.zeros((OFF, 128), F32)
    headx[tile_rows(TILES, 0, ROWS), :] = jnp.zeros((ROWS, 128), F32)
    lhs[...] = jnp.zeros_like(lhs)
    part[...] = jnp.zeros_like(part)
    moves[0].wait()
    blocks = blk_v[...]
    index8[...] = (blocks & 7) * EXT + (blocks >> 3) + OFF
    listed = pltpu.make_async_copy(index8, index_s, sems.at[16])
    listed.start()
    moves[1].wait()
    reach8 = reach_v[...]
    slot8 = (((reach8 // REACH) % 16 - base + 16) % 16) * REACH + reach8 % REACH
    lane = lax.broadcasted_iota(I32, (128, 128), 1)
    for k in range(SEG // 128):
        slots = column_of(slot8[k : k + 1, :])
        for q in range(FRAME // 128):
            oh[k * 128 : (k + 1) * 128, q * 128 : (q + 1) * 128] = jnp.where(
                slots == lane + q * 128, 1.0, 0.0
            ).astype(BF16)
    for m in moves[2:]:
        m.wait()
    nets = net_v[...]
    inflow = jnp.zeros(nets.shape, F32)
    for n in range(NETS):
        inflow = jnp.where(nets == n, infl_s[n], inflow)
    values = (bed_v[...], inflow, sec0_v[...])
    odd = j % 2
    for w in range(2):
        keep = odd == w
        for t in range(2):
            at = (1 + w) * REACH + t * 128
            for q, v in enumerate(values):
                part[2 + q : 3 + q, at : at + 128] = jnp.where(keep, v[t : t + 1, :], 0.0)
    weight[...] = mask_v[...].astype(F32) * cond_v[...]
    row_sums(lambda at: weight[at, :], lhs, 3)
    listed.wait()
    for m in heads:
        m.wait()
    gather_rows(headx, index_s, hs)
    row_sums(lambda at: weight[at, :] * hs[at, :], lhs, 0)
    sums = jnp.dot(lhs[...].astype(BF16), oh[...], preferred_element_type=F32)
    part[0:1, :] = sums[0:1] + sums[1:2] + sums[2:3]
    part[1:2, :] = sums[3:4] + sums[4:5] + sums[5:6]


def fields(headx, recharge, storage, index8, weight, onehot, inv, supply, rech_v, store_v, sems):
    moves = [
        pltpu.make_async_copy(recharge, rech_v, sems.at[0]),
        pltpu.make_async_copy(storage, store_v, sems.at[1]),
    ]
    for m in moves:
        m.start()
    target = index8[...]
    iota = lax.broadcasted_iota(I32, (ROWS, 128), 0)
    for k in range(SEG // 128):
        row = jnp.broadcast_to(target[k : k + 1, :], (ROWS, 128))
        for c in range(TILES):
            onehot[c * ROWS : (c + 1) * ROWS, k * 128 : (k + 1) * 128] = jnp.where(
                row == iota + (c * EXT + OFF), 1.0, 0.0
            ).astype(BF16)
    both = both_halves(weight[...])
    inv[TILES] = jnp.zeros((ROWS, 128), F32)
    for m in moves:
        m.wait()
    for c in range(TILES):
        at = slice(c * 128, (c + 1) * 128)
        got = jnp.dot(onehot[c * ROWS : (c + 1) * ROWS, :], both, preferred_element_type=F32)
        cond = got[:, :128] + got[:, 128:]
        store = store_v[:, at]
        inv[c] = 1.0 / (4.0 + store + cond)
        supply[c] = store * headx[tile_rows(c, 0, ROWS), :] + rech_v[:, at]


def put_columns(left_tile, right_tile, q, ma, mb):
    odd = lax.axis_index("col") % 2 == 1
    for k in range(ROWS // 128):
        at = slice(k * 128, (k + 1) * 128)
        left = left_tile(at).T[0:H, :]
        right = right_tile(at).T[128 - H : 128, :]
        ma[q * H : (q + 1) * H, at] = jnp.where(odd, left, right)
        mb[q * H : (q + 1) * H, at] = jnp.where(odd, right, left)


def columns(first, *refs):
    head = refs[0]
    ma, mb = refs[-2:]
    ma[...] = jnp.zeros_like(ma)
    mb[...] = jnp.zeros_like(mb)
    put_columns(
        lambda at: head[tile_rows(0, at.start, 128), :],
        lambda at: head[tile_rows(TILES - 1, at.start, 128), :],
        0, ma, mb,
    )
    if first:
        inv = refs[1]
        put_columns(lambda at: inv[0, at, :], lambda at: inv[TILES - 1, at, :], 2, ma, mb)


def section_kernel(first, *refs):
    if first:
        own, up, down, oh, onehot, weight, supply, pa, pb, frame, section, mixed, rhs, ma, mb = refs
    else:
        own, up, down, old, oh, onehot, weight, supply, pa, pb, section, mixed, rhs, ma, mb = refs
    j = lax.axis_index("col")
    full = own[...] + jnp.concatenate([up[...], down[...]], axis=1)
    leak = full[0:1]
    if first:
        wsum, bed, inflow, sec = full[1:2], full[2:3], full[3:4], full[4:5]
    else:
        wsum, bed, inflow, sec = (old[q : q + 1, :] for q in (1, 2, 3, 4))
    x = inflow - (sec * wsum - leak)
    soft = jnp.maximum(x, 0.0) + jnp.log1p(jnp.exp(-jnp.abs(x)))
    sec = bed + jnp.sqrt(1.0 + soft) - 1.0
    if first:
        frame[...] = full
        frame[4:5, :] = sec
    odd = j % 2 == 1
    for t in range(2):
        a = REACH + t * 128
        b = 2 * REACH + t * 128
        section[t : t + 1, :] = jnp.where(odd, sec[:, b : b + 128], sec[:, a : a + 128])
    hi, lo = split2(sec)
    wide = jnp.concatenate(
        [jnp.broadcast_to(hi.astype(F32), (128, FRAME)), jnp.broadcast_to(lo.astype(F32), (128, FRAME))], axis=0
    ).astype(BF16)
    got = lax.dot_general(oh[...], wide, (((1,), (1,)), ((), ())), preferred_element_type=F32)
    both = both_halves(weight[...] * (got[:, :128] + got[:, 128:]))
    mixed[...] = both
    ma[...] = pa[...]
    mb[...] = pb[...]
    for c in (0, TILES - 1):
        scatter(c, onehot, both, supply, rhs)
    put_columns(lambda at: rhs[0, at, :], lambda at: rhs[TILES - 1, at, :], 1, ma, mb)


def scatter(c, onehot, both, supply, rhs):
    got = jnp.dot(onehot[c * ROWS : (c + 1) * ROWS, :], both, preferred_element_type=F32)
    rhs[c] = supply[c] + got[:, :128] + got[:, 128:]


def inner_source(onehot, mixed, supply, rhs_in, rhs):
    both = mixed[...]
    for c in range(1, TILES - 1):
        scatter(c, onehot, both, supply, rhs)


def place_columns(first, *refs):
    if first:
        ca, cb, _, _, _, head, rhs, inv, sa, sb, band, wide = refs
        grids = (rhs, inv)
    else:
        ca, cb, _, _, head, rhs, sa, sb, band, wide = refs
        grids = (rhs,)
    i = lax.axis_index("row")
    j = lax.axis_index("col")
    odd = j % 2 == 1
    right = jnp.where(j == 15, 0.0, jnp.where(odd, cb[...], ca[...]))
    left = jnp.where(j == 0, 0.0, jnp.where(odd, ca[...], cb[...]))
    wide[...] = jnp.zeros_like(wide)
    row_odd = i % 2 == 1
    sa[...] = jnp.zeros_like(sa)
    sb[...] = jnp.zeros_like(sb)
    for q in range(1 + len(grids)):
        own = slice(q * H, (q + 1) * H)
        wide[0:H, :] = right[own, :]
        wide[128 - H : 128, :] = left[own, :]
        for k in range(ROWS // 128):
            turned = wide[:, k * 128 : (k + 1) * 128].T
            if q == 0:
                head[tile_rows(TILES, k * 128, 128), :] = turned
            else:
                grids[q - 1][TILES, k * 128 : (k + 1) * 128, :] = turned
        depth = DEPTH[q]
        for c in range(WIDE):
            if q == 0:
                top = head[tile_rows(c, 0, depth), :]
                bottom = head[tile_rows(c, ROWS - depth, depth), :]
            else:
                ref = grids[q - 1]
                top = ref[c, 0:depth, :]
                bottom = ref[c, ROWS - depth : ROWS, :]
            at = strip_rows(c, q, 1 + len(grids))
            sa[at, :] = jnp.where(row_odd, top, bottom)
            sb[at, :] = jnp.where(row_odd, bottom, top)
    for c in range(WIDE):
        band[0, c] = head[tile_rows(c, 0, 8), :]
        band[1, c] = head[tile_rows(c, ROWS - 8, 8), :]


def strip_rows(c, q, count):
    first = c * sum(DEPTH[:count]) + sum(DEPTH[:q])
    return slice(first, first + DEPTH[q])


def halo_rows(ra, rb, q, count, top, bottom):
    i = lax.axis_index("row")
    odd = i % 2 == 1
    for c in range(WIDE):
        at = strip_rows(c, q, count)
        a, b = ra[at, :], rb[at, :]
        top(c, jnp.where(i == 0, 0.0, jnp.where(odd, a, b)))
        bottom(c, jnp.where(i == 15, 0.0, jnp.where(odd, b, a)))


def relax_chunk(src, dst, rhs, inv, spread):
    lane = lax.broadcasted_iota(I32, (8, 128), 1)
    mid = [src(c, 0) for c in range(WIDE)]
    fwd = [pltpu.roll(m, 1, 1) for m in mid]
    bwd = [pltpu.roll(m, 127, 1) for m in mid]
    for c in range(spread):
        left = jnp.where(lane == 0, fwd[c - 1], fwd[c])
        right = jnp.where(lane == 127, bwd[(c + 1) % WIDE], bwd[c])
        total = (src(c, -1) + src(c, 1)) + (left + right) + rhs(c)
        dst(c, total * inv(c))


def sweep(src, dst, rhs, inv):
    def put(c, r, value):
        dst[pl.ds(c * EXT + OFF + r, 8), :] = value

    def group(g, carry):
        for u in range(UNROLL):
            r = g * (8 * UNROLL) + u * 8
            relax_chunk(
                lambda c, d: src[pl.ds(c * EXT + OFF + r + d, 8), :],
                lambda c, value: put(c, r, value),
                lambda c: rhs[c, pl.ds(r, 8), :],
                lambda c: inv[c, pl.ds(r, 8), :],
                WIDE,
            )
        return carry

    lax.fori_loop(0, ROWS // (8 * UNROLL), group, 0)


def sweeps(head, other, rhs, inv):
    for c in range(WIDE):
        other[c * EXT : c * EXT + OFF, :] = jnp.zeros((OFF, 128), F32)
        other[(c + 1) * EXT - OFF : (c + 1) * EXT, :] = jnp.zeros((OFF, 128), F32)
    for _ in range(SWEEPS // 2):
        sweep(head, other, rhs, inv)
        sweep(other, head, rhs, inv)


def inner_relax(head_in, rhs, inv, head, other):
    sweeps(head, other, rhs, inv)


def band_relax(ra, rb, count, band, get_rhs, get_inv, one, two):
    one[...] = jnp.zeros_like(one)
    two[...] = jnp.zeros_like(two)
    for c in range(WIDE):
        one[0, c, 16:24, :] = band[0, c]
        one[1, c, 8:16, :] = band[1, c]

    def top(c, value):
        one[0, c, 16 - H : 16, :] = value

    def bottom(c, value):
        one[1, c, 16 : 16 + H, :] = value

    halo_rows(ra, rb, 0, count, top, bottom)
    src, dst = one, two
    for _ in range(SWEEPS):
        for side in range(2):
            for t in range(2):
                r = 8 + t * 8

                def put(c, value):
                    dst[side, c, r : r + 8, :] = value

                relax_chunk(
                    lambda c, d: src[side, c, r + d : r + d + 8, :],
                    put,
                    lambda c: get_rhs(side, c, t),
                    lambda c: get_inv(side, c, t),
                    WIDE,
                )
        src, dst = dst, src
    return one


def halo_or_own(ref, spare):
    def get(side, c, t):
        if side == 0:
            return ref[c, 0:8, :] if t == 1 else spare[0, c]
        return ref[c, ROWS - 8 : ROWS, :] if t == 0 else spare[1, c]

    return get


def fill_spare(ra, rb, q, count, spare):
    spare[...] = jnp.zeros_like(spare)

    def top(c, value):
        spare[0, c, 8 - DEPTH[q] : 8, :] = value

    def bottom(c, value):
        spare[1, c, 0 : DEPTH[q], :] = value

    halo_rows(ra, rb, q, count, top, bottom)


def finish_first(
    ra, rb, band, head_in, rhs, inv, index8, weight, oh, head, rim, part, one, two, hs, lhs, spare, index_s, sem
):
    listed = pltpu.make_async_copy(index8, index_s, sem)
    listed.start()
    fill_spare(ra, rb, 1, 3, spare)
    fill_spare(ra, rb, 2, 3, rim)
    done = band_relax(ra, rb, 3, band, halo_or_own(rhs, spare), halo_or_own(inv, rim), one, two)
    for c in range(TILES):
        head[tile_rows(c, 0, H), :] = done[0, c, 16 : 16 + H, :]
        head[tile_rows(c, ROWS - H, H), :] = done[1, c, 16 - H : 16, :]
    listed.wait()
    lhs[...] = jnp.zeros_like(lhs)
    gather_rows(head, index_s, hs)
    row_sums(lambda at: weight[at, :] * hs[at, :], lhs, 0)
    sums = jnp.dot(lhs[...].astype(BF16), oh[...], preferred_element_type=F32)
    part[...] = jnp.zeros_like(part)
    part[0:1, :] = sums[0:1] + sums[1:2] + sums[2:3]


def finish_last(ra, rb, band, head, rhs, inv, rim, out, one, two, spare, edge, sems):
    moves = [
        pltpu.make_async_copy(
            head.at[tile_rows(c, 8, ROWS - 16), :], out.at[8 : ROWS - 8, c * 128 : (c + 1) * 128], sems.at[2 + c]
        )
        for c in range(TILES)
    ]
    for m in moves:
        m.start()
    fill_spare(ra, rb, 1, 2, spare)
    done = band_relax(ra, rb, 2, band, halo_or_own(rhs, spare), halo_or_own(inv, rim), one, two)
    for c in range(TILES):
        at = slice(c * 128, (c + 1) * 128)
        edge[0, :, at] = head[tile_rows(c, 0, 8), :]
        edge[1, :, at] = head[tile_rows(c, ROWS - 8, 8), :]
        edge[0, 0:H, at] = done[0, c, 16 : 16 + H, :]
        edge[1, 8 - H : 8, at] = done[1, c, 16 - H : 16, :]
    edges = [
        pltpu.make_async_copy(edge.at[0], out.at[0:8, :], sems.at[0]),
        pltpu.make_async_copy(edge.at[1], out.at[ROWS - 8 : ROWS, :], sems.at[1]),
    ]
    for m in edges:
        m.start()
    for m in moves + edges:
        m.wait()


def shape(*dims, dtype=F32):
    return jax.ShapeDtypeStruct(dims, dtype)


def far(x):
    return pltpu.with_memory_space_constraint(x, pltpu.HBM)


def call(kernel, outs, ins, scratch=(), hbm=(), hbm_out=(), aliases=None, limit=16, flops=10_000_000):
    def at(k, far):
        return pl.BlockSpec(memory_space=pltpu.HBM if k in far else pltpu.VMEM)

    return pl.pallas_call(
        kernel,
        out_shape=outs,
        in_specs=[at(k, hbm) for k in range(len(ins))],
        out_specs=tuple(at(k, hbm_out) for k in range(len(outs))),
        scratch_shapes=list(scratch),
        input_output_aliases=aliases or {},
        compiler_params=pltpu.CompilerParams(vmem_limit_bytes=limit * 2**20),
        cost_estimate=pl.CostEstimate(flops=flops, bytes_accessed=4_000_000, transcendentals=0),
    )(*[far(x) if k in hbm else x for k, x in enumerate(ins)])


def swap(x, axis, which):
    n = lax.axis_size(axis)
    if which == 0:
        pairs = [(k, k ^ 1) for k in range(n)]
    else:
        pairs = [(k, (k + 1) % n if k % 2 else (k - 1) % n) for k in range(n)]
    return lax.ppermute(x, axis, pairs)


def swap_both(a, b, axis):
    b = swap(b, axis, 1)
    a = swap(a, axis, 0)
    return a, b


def shift(x, axis, by):
    n = lax.axis_size(axis)
    return lax.ppermute(x, axis, [(k, (k + by) % n) for k in range(n)])


def exchange_sums(part):
    both = part + swap(part, "col", 0)
    up = shift(both[:, 2 * REACH :], "col", 2)
    down = shift(both[:, : 2 * REACH], "col", -2)
    return both, up, down


EXT_SHAPE = shape(WIDE * EXT, 128)
GRID = shape(WIDE, ROWS, 128)
BAND = shape(2, WIDE, 8, 128)
SEG_ROWS = pltpu.VMEM((SEG, 128), F32)
SUMS = pltpu.VMEM((16, SEG), F32)
OTHER = pltpu.VMEM((WIDE * EXT, 128), F32)
WORK = pltpu.VMEM((2, WIDE, 32, 128), F32)
SPARE = pltpu.VMEM((2, WIDE, 8, 128), F32)
TURN = pltpu.VMEM((128, ROWS), F32)
SMALL = pltpu.SMEM((8, 128), I32)


def sems(n):
    return pltpu.SemaphoreType.DMA((n,))


def body(head0, recharge, storage, seg_block, seg_mask, seg_cond, seg_reach, bed, sec0, net, infl):
    part, oh, weight, head, index8 = call(
        prep,
        (shape(8, FRAME), shape(SEG, FRAME, dtype=BF16), shape(SEG, 128), EXT_SHAPE, shape(8, 128, dtype=I32)),
        (
            head0,
            seg_block.reshape(8, 128),
            seg_reach.reshape(8, 128),
            seg_mask,
            seg_cond,
            bed.reshape(2, 128),
            sec0.reshape(2, 128),
            net.reshape(2, 128),
            infl,
        ),
        scratch=[
            SEG_ROWS,
            SUMS,
            pltpu.VMEM((8, 128), I32),
            pltpu.VMEM((8, 128), I32),
            pltpu.VMEM((SEG, 128), I32),
            SEG_ROWS,
            pltpu.VMEM((2, 128), F32),
            pltpu.VMEM((2, 128), F32),
            pltpu.VMEM((2, 128), I32),
            pltpu.SMEM((NETS,), F32),
            SMALL,
            sems(17),
        ],
        hbm=range(9),
    )
    own, up, down = exchange_sums(part)
    onehot, inv, supply = call(
        fields,
        (shape(TILES * ROWS, SEG, dtype=BF16), GRID, shape(TILES, ROWS, 128)),
        (head, recharge, storage, index8, weight),
        scratch=[pltpu.VMEM((ROWS, COLS), F32), pltpu.VMEM((ROWS, COLS), F32), sems(2)],
        hbm=(1, 2),
    )
    strip = shape(16, ROWS)
    pa, pb = call(functools.partial(columns, True), (strip, strip), (head, inv))
    mixed_shape = shape(SEG, 256, dtype=BF16)
    frame, section, mixed, rhs, ma, mb = call(
        functools.partial(section_kernel, True),
        (shape(8, FRAME), shape(2, 128), mixed_shape, GRID, strip, strip),
        (own, up, down, oh, onehot, weight, supply, pa, pb),
    )
    ca, cb = swap_both(ma, mb, "col")
    (rhs,) = call(inner_source, (GRID,), (onehot, mixed, supply, rhs), aliases={3: 0})
    rows = shape(96, 128)
    head, rhs, inv, sa, sb, band = call(
        functools.partial(place_columns, True),
        (EXT_SHAPE, GRID, GRID, rows, rows, BAND),
        (ca, cb, head, rhs, inv),
        scratch=[TURN],
        aliases={2: 0, 3: 1, 4: 2},
    )
    ra, rb = swap_both(sa, sb, "row")
    (head,) = call(inner_relax, (EXT_SHAPE,), (head, rhs, inv), scratch=[OTHER], aliases={0: 0})
    head, rim, part = call(
        finish_first,
        (EXT_SHAPE, BAND, shape(8, FRAME)),
        (ra, rb, band, head, rhs, inv, index8, weight, oh),
        scratch=[WORK, WORK, SEG_ROWS, SUMS, SPARE, SMALL, pltpu.SemaphoreType.DMA],
        aliases={3: 0},
    )
    own, up, down = exchange_sums(part)
    strip = shape(8, ROWS)
    pa, pb = call(functools.partial(columns, False), (strip, strip), (head,))
    section, mixed, rhs, ma, mb = call(
        functools.partial(section_kernel, False),
        (shape(2, 128), mixed_shape, GRID, strip, strip),
        (own, up, down, frame, oh, onehot, weight, supply, pa, pb),
    )
    ca, cb = swap_both(ma, mb, "col")
    (rhs,) = call(inner_source, (GRID,), (onehot, mixed, supply, rhs), aliases={3: 0})
    rows = shape(64, 128)
    head, rhs, sa, sb, band = call(
        functools.partial(place_columns, False),
        (EXT_SHAPE, GRID, rows, rows, BAND),
        (ca, cb, head, rhs),
        scratch=[TURN],
        aliases={2: 0, 3: 1},
    )
    ra, rb = swap_both(sa, sb, "row")
    (head,) = call(inner_relax, (EXT_SHAPE,), (head, rhs, inv), scratch=[OTHER], aliases={0: 0})
    (out,) = call(
        finish_last,
        (shape(ROWS, COLS),),
        (ra, rb, band, head, rhs, inv, rim),
        scratch=[WORK, WORK, SPARE, pltpu.VMEM((2, 8, COLS), F32), sems(2 + TILES)],
        hbm_out=(0,),
    )
    return out, section.reshape(REACH)


def solution(mesh):
    placed = (
        P("row", "col"),
        P("row", "col"),
        P("row", "col"),
        P(("row", "col")),
        P(("row", "col"), None),
        P(("row", "col"), None),
        P(("row", "col")),
        P(("row", "col")),
        P(("row", "col")),
        P(("row", "col")),
        P(),
    )
    return jax.shard_map(
        body,
        mesh=mesh,
        in_specs=placed,
        out_specs=(P("row", "col"), P(("row", "col"))),
        check_vma=False,
    )
```

```python
import functools

import jax
import jax.numpy as jnp
from jax import lax
from jax.experimental import pallas as pl
from jax.experimental.pallas import tpu as pltpu
from jax.sharding import PartitionSpec as P

NETS = 64
SWEEPS = 4
ROWS, COLS = 384, 1024
TILES = COLS // 128
WIDE = TILES + 1
SEG = 1024
REACH = 256
FRAME = 4 * REACH
LOCAL = 3 * REACH
OFF = 8
EXT = ROWS + 2 * OFF
H = 4
DEPTH = (4, 3, 3)
UNROLL = 12
F32 = jnp.float32
BF16 = jnp.bfloat16
I32 = jnp.int32


def split2(x):
    hi = x.astype(BF16)
    lo = (x - hi.astype(F32)).astype(BF16)
    return hi, lo


def both_halves(x):
    return jnp.concatenate(split2(x), axis=1)


def column_of(row):
    return jnp.broadcast_to(row, (128, 128)).T


def tile_rows(c, start, size):
    return slice(c * EXT + OFF + start, c * EXT + OFF + start + size)


def gather_rows(head, index, out):
    def group(k, carry):
        for u in range(128):
            out[pl.ds(k * 128 + u, 1), :] = head[pl.ds(index[k, u], 1), :]
        return carry

    lax.fori_loop(0, SEG // 128, group, 0)


def row_sums(get, lhs, first):
    for k in range(SEG // 128):
        at = slice(k * 128, (k + 1) * 128)
        row = jnp.sum(get(at).T, axis=0, keepdims=True)
        hi = row.astype(BF16).astype(F32)
        mid = (row - hi).astype(BF16).astype(F32)
        lhs[first : first + 1, at] = hi
        lhs[first + 1 : first + 2, at] = mid
        lhs[first + 2 : first + 3, at] = row - hi - mid


def to_frame(row):
    odd = lax.axis_index("col") % 2 == 1
    parts = [row[:, m * REACH : (m + 1) * REACH] for m in range(3)]
    none = jnp.zeros_like(parts[0])
    pairs = zip([none] + parts, parts + [none])
    return jnp.concatenate([jnp.where(odd, a, b) for a, b in pairs], axis=1)


def to_local(row):
    odd = lax.axis_index("col") % 2 == 1
    parts = [row[:, m * REACH : (m + 1) * REACH] for m in range(4)]
    return jnp.concatenate([jnp.where(odd, b, a) for a, b in zip(parts[:3], parts[1:])], axis=1)


def prep(
    head, blk, reach, mask, condu, bed, sec0, net, infl,
    part, oh, weight, headx, index8,
    hs, lhs, blk_v, reach_v, mask_v, cond_v, bed_v, sec0_v, net_v, infl_s, index_s, sems,
):
    moves = [
        pltpu.make_async_copy(blk, blk_v, sems.at[0]),
        pltpu.make_async_copy(reach, reach_v, sems.at[1]),
        pltpu.make_async_copy(mask, mask_v, sems.at[2]),
        pltpu.make_async_copy(condu, cond_v, sems.at[3]),
        pltpu.make_async_copy(bed, bed_v, sems.at[4]),
        pltpu.make_async_copy(sec0, sec0_v, sems.at[5]),
        pltpu.make_async_copy(net, net_v, sems.at[6]),
        pltpu.make_async_copy(infl, infl_s, sems.at[7]),
    ]
    heads = [
        pltpu.make_async_copy(
            head.at[:, c * 128 : (c + 1) * 128], headx.at[tile_rows(c, 0, ROWS), :], sems.at[8 + c]
        )
        for c in range(TILES)
    ]
    for m in moves + heads:
        m.start()
    j = lax.axis_index("col")
    base = j - 1
    for c in range(WIDE):
        headx[c * EXT : c * EXT + OFF, :] = jnp.zeros((OFF, 128), F32)
        headx[(c + 1) * EXT - OFF : (c + 1) * EXT, :] = jnp.zeros((OFF, 128), F32)
    headx[tile_rows(TILES, 0, ROWS), :] = jnp.zeros((ROWS, 128), F32)
    lhs[...] = jnp.zeros_like(lhs)
    part[...] = jnp.zeros_like(part)
    moves[0].wait()
    blocks = blk_v[...]
    index8[...] = (blocks & 7) * EXT + (blocks >> 3) + OFF
    listed = pltpu.make_async_copy(index8, index_s, sems.at[16])
    listed.start()
    moves[1].wait()
    reach8 = reach_v[...]
    slot8 = (((reach8 // REACH) % 16 - base + 16) % 16) * REACH + reach8 % REACH
    lane = lax.broadcasted_iota(I32, (128, 128), 1)
    for k in range(SEG // 128):
        slots = column_of(slot8[k : k + 1, :])
        for q in range(LOCAL // 128):
            oh[k * 128 : (k + 1) * 128, q * 128 : (q + 1) * 128] = jnp.where(
                slots == lane + q * 128, 1.0, 0.0
            ).astype(BF16)
    for m in moves[2:]:
        m.wait()
    nets = net_v[...]
    inflow = jnp.zeros(nets.shape, F32)
    for n in range(NETS):
        inflow = jnp.where(nets == n, infl_s[n], inflow)
    values = (bed_v[...], inflow, sec0_v[...])
    odd = j % 2
    for w in range(2):
        keep = odd == w
        for t in range(2):
            at = (1 + w) * REACH + t * 128
            for q, v in enumerate(values):
                part[2 + q : 3 + q, at : at + 128] = jnp.where(keep, v[t : t + 1, :], 0.0)
    weight[...] = mask_v[...].astype(F32) * cond_v[...]
    row_sums(lambda at: weight[at, :], lhs, 3)
    listed.wait()
    for m in heads:
        m.wait()
    gather_rows(headx, index_s, hs)
    row_sums(lambda at: weight[at, :] * hs[at, :], lhs, 0)
    sums = jnp.dot(lhs[...].astype(BF16), oh[...], preferred_element_type=F32)
    part[0:1, :] = to_frame(sums[0:1] + sums[1:2] + sums[2:3])
    part[1:2, :] = to_frame(sums[3:4] + sums[4:5] + sums[5:6])


def fields(headx, recharge, storage, index8, weight, onehot, inv, supply, rech_v, store_v, sems):
    moves = [
        pltpu.make_async_copy(recharge, rech_v, sems.at[0]),
        pltpu.make_async_copy(storage, store_v, sems.at[1]),
    ]
    for m in moves:
        m.start()
    target = index8[...]
    iota = lax.broadcasted_iota(I32, (ROWS, 128), 0)
    for k in range(SEG // 128):
        row = jnp.broadcast_to(target[k : k + 1, :], (ROWS, 128))
        for c in range(TILES):
            onehot[c * ROWS : (c + 1) * ROWS, k * 128 : (k + 1) * 128] = jnp.where(
                row == iota + (c * EXT + OFF), 1.0, 0.0
            ).astype(BF16)
    both = both_halves(weight[...])
    inv[TILES] = jnp.zeros((ROWS, 128), F32)
    for m in moves:
        m.wait()
    for c in range(TILES):
        at = slice(c * 128, (c + 1) * 128)
        got = jnp.dot(onehot[c * ROWS : (c + 1) * ROWS, :], both, preferred_element_type=F32)
        cond = got[:, :128] + got[:, 128:]
        store = store_v[:, at]
        inv[c] = 1.0 / (4.0 + store + cond)
        supply[c] = store * headx[tile_rows(c, 0, ROWS), :] + rech_v[:, at]


def put_columns(left_tile, right_tile, q, ma, mb):
    odd = lax.axis_index("col") % 2 == 1
    for k in range(ROWS // 128):
        at = slice(k * 128, (k + 1) * 128)
        left = left_tile(at).T[0:H, :]
        right = right_tile(at).T[128 - H : 128, :]
        ma[q * H : (q + 1) * H, at] = jnp.where(odd, left, right)
        mb[q * H : (q + 1) * H, at] = jnp.where(odd, right, left)


def columns(first, *refs):
    head = refs[0]
    ma, mb = refs[-2:]
    ma[...] = jnp.zeros_like(ma)
    mb[...] = jnp.zeros_like(mb)
    put_columns(
        lambda at: head[tile_rows(0, at.start, 128), :],
        lambda at: head[tile_rows(TILES - 1, at.start, 128), :],
        0, ma, mb,
    )
    if first:
        inv = refs[1]
        put_columns(lambda at: inv[0, at, :], lambda at: inv[TILES - 1, at, :], 2, ma, mb)


def section_kernel(first, *refs):
    if first:
        own, up, down, oh, onehot, weight, supply, pa, pb, frame, mixed, rhs, ma, mb = refs
    else:
        own, up, down, old, oh, onehot, weight, supply, pa, pb, reaches, mixed, rhs, ma, mb = refs
    full = own[...] + jnp.concatenate([up[...], down[...]], axis=1)
    leak = full[0:1]
    if first:
        wsum, bed, inflow, sec = full[1:2], full[2:3], full[3:4], full[4:5]
    else:
        wsum, bed, inflow, sec = (old[q : q + 1, :] for q in (1, 2, 3, 4))
    x = inflow - (sec * wsum - leak)
    soft = jnp.maximum(x, 0.0) + jnp.log1p(jnp.exp(-jnp.abs(x)))
    sec = bed + jnp.sqrt(1.0 + soft) - 1.0
    if first:
        frame[...] = full
        frame[4:5, :] = sec
    else:
        reaches[...] = sec
    hi, lo = split2(to_local(sec))
    wide = jnp.concatenate(
        [jnp.broadcast_to(hi.astype(F32), (128, LOCAL)), jnp.broadcast_to(lo.astype(F32), (128, LOCAL))], axis=0
    ).astype(BF16)
    got = lax.dot_general(oh[...], wide, (((1,), (1,)), ((), ())), preferred_element_type=F32)
    both = both_halves(weight[...] * (got[:, :128] + got[:, 128:]))
    mixed[...] = both
    ma[...] = pa[...]
    mb[...] = pb[...]
    for c in (0, TILES - 1):
        scatter(c, onehot, both, supply, rhs)
    put_columns(lambda at: rhs[0, at, :], lambda at: rhs[TILES - 1, at, :], 1, ma, mb)


def scatter(c, onehot, both, supply, rhs):
    got = jnp.dot(onehot[c * ROWS : (c + 1) * ROWS, :], both, preferred_element_type=F32)
    rhs[c] = supply[c] + got[:, :128] + got[:, 128:]


def inner_source(onehot, mixed, supply, rhs_in, rhs):
    both = mixed[...]
    for c in range(1, TILES - 1):
        scatter(c, onehot, both, supply, rhs)


def place_columns(first, *refs):
    if first:
        ca, cb, _, _, _, head, rhs, inv, sa, sb, band, wide = refs
        grids = (rhs, inv)
    else:
        ca, cb, _, _, head, rhs, sa, sb, band, wide = refs
        grids = (rhs,)
    i = lax.axis_index("row")
    j = lax.axis_index("col")
    odd = j % 2 == 1
    right = jnp.where(j == 15, 0.0, jnp.where(odd, cb[...], ca[...]))
    left = jnp.where(j == 0, 0.0, jnp.where(odd, ca[...], cb[...]))
    wide[...] = jnp.zeros_like(wide)
    row_odd = i % 2 == 1
    sa[...] = jnp.zeros_like(sa)
    sb[...] = jnp.zeros_like(sb)
    for q in range(1 + len(grids)):
        own = slice(q * H, (q + 1) * H)
        wide[0:H, :] = right[own, :]
        wide[128 - H : 128, :] = left[own, :]
        for k in range(ROWS // 128):
            turned = wide[:, k * 128 : (k + 1) * 128].T
            if q == 0:
                head[tile_rows(TILES, k * 128, 128), :] = turned
            else:
                grids[q - 1][TILES, k * 128 : (k + 1) * 128, :] = turned
        depth = DEPTH[q]
        for c in range(WIDE):
            if q == 0:
                top = head[tile_rows(c, 0, depth), :]
                bottom = head[tile_rows(c, ROWS - depth, depth), :]
            else:
                ref = grids[q - 1]
                top = ref[c, 0:depth, :]
                bottom = ref[c, ROWS - depth : ROWS, :]
            at = strip_rows(c, q, 1 + len(grids))
            sa[at, :] = jnp.where(row_odd, top, bottom)
            sb[at, :] = jnp.where(row_odd, bottom, top)
    for c in range(WIDE):
        band[0, c] = head[tile_rows(c, 0, 8), :]
        band[1, c] = head[tile_rows(c, ROWS - 8, 8), :]


def strip_rows(c, q, count):
    first = c * sum(DEPTH[:count]) + sum(DEPTH[:q])
    return slice(first, first + DEPTH[q])


def halo_rows(ra, rb, q, count, top, bottom):
    i = lax.axis_index("row")
    odd = i % 2 == 1
    for c in range(WIDE):
        at = strip_rows(c, q, count)
        a, b = ra[at, :], rb[at, :]
        top(c, jnp.where(i == 0, 0.0, jnp.where(odd, a, b)))
        bottom(c, jnp.where(i == 15, 0.0, jnp.where(odd, b, a)))


def relax_chunk(src, dst, rhs, inv, spread):
    lane = lax.broadcasted_iota(I32, (8, 128), 1)
    mid = [src(c, 0) for c in range(WIDE)]
    fwd = [pltpu.roll(m, 1, 1) for m in mid]
    bwd = [pltpu.roll(m, 127, 1) for m in mid]
    for c in range(spread):
        left = jnp.where(lane == 0, fwd[c - 1], fwd[c])
        right = jnp.where(lane == 127, bwd[(c + 1) % WIDE], bwd[c])
        total = (src(c, -1) + src(c, 1)) + (left + right) + rhs(c)
        dst(c, total * inv(c))


def sweep(src, dst, rhs, inv):
    def put(c, r, value):
        dst[pl.ds(c * EXT + OFF + r, 8), :] = value

    def group(g, carry):
        for u in range(UNROLL):
            r = g * (8 * UNROLL) + u * 8
            relax_chunk(
                lambda c, d: src[pl.ds(c * EXT + OFF + r + d, 8), :],
                lambda c, value: put(c, r, value),
                lambda c: rhs[c, pl.ds(r, 8), :],
                lambda c: inv[c, pl.ds(r, 8), :],
                WIDE,
            )
        return carry

    lax.fori_loop(0, ROWS // (8 * UNROLL), group, 0)


def sweeps(head, other, rhs, inv):
    for c in range(WIDE):
        other[c * EXT : c * EXT + OFF, :] = jnp.zeros((OFF, 128), F32)
        other[(c + 1) * EXT - OFF : (c + 1) * EXT, :] = jnp.zeros((OFF, 128), F32)
    for _ in range(SWEEPS // 2):
        sweep(head, other, rhs, inv)
        sweep(other, head, rhs, inv)


def inner_relax(head_in, rhs, inv, head, other):
    sweeps(head, other, rhs, inv)


def band_relax(ra, rb, count, band, get_rhs, get_inv, one, two):
    one[...] = jnp.zeros_like(one)
    two[...] = jnp.zeros_like(two)
    for c in range(WIDE):
        one[0, c, 16:24, :] = band[0, c]
        one[1, c, 8:16, :] = band[1, c]

    def top(c, value):
        one[0, c, 16 - H : 16, :] = value

    def bottom(c, value):
        one[1, c, 16 : 16 + H, :] = value

    halo_rows(ra, rb, 0, count, top, bottom)
    src, dst = one, two
    for _ in range(SWEEPS):
        for side in range(2):
            for t in range(2):
                r = 8 + t * 8

                def put(c, value):
                    dst[side, c, r : r + 8, :] = value

                relax_chunk(
                    lambda c, d: src[side, c, r + d : r + d + 8, :],
                    put,
                    lambda c: get_rhs(side, c, t),
                    lambda c: get_inv(side, c, t),
                    WIDE,
                )
        src, dst = dst, src
    return one


def halo_or_own(ref, spare):
    def get(side, c, t):
        if side == 0:
            return ref[c, 0:8, :] if t == 1 else spare[0, c]
        return ref[c, ROWS - 8 : ROWS, :] if t == 0 else spare[1, c]

    return get


def fill_spare(ra, rb, q, count, spare):
    spare[...] = jnp.zeros_like(spare)

    def top(c, value):
        spare[0, c, 8 - DEPTH[q] : 8, :] = value

    def bottom(c, value):
        spare[1, c, 0 : DEPTH[q], :] = value

    halo_rows(ra, rb, q, count, top, bottom)


def finish_first(
    ra, rb, band, head_in, rhs, inv, index8, weight, oh, head, rim, part, one, two, hs, lhs, spare, index_s, sem
):
    listed = pltpu.make_async_copy(index8, index_s, sem)
    listed.start()
    fill_spare(ra, rb, 1, 3, spare)
    fill_spare(ra, rb, 2, 3, rim)
    done = band_relax(ra, rb, 3, band, halo_or_own(rhs, spare), halo_or_own(inv, rim), one, two)
    for c in range(TILES):
        head[tile_rows(c, 0, H), :] = done[0, c, 16 : 16 + H, :]
        head[tile_rows(c, ROWS - H, H), :] = done[1, c, 16 - H : 16, :]
    listed.wait()
    lhs[...] = jnp.zeros_like(lhs)
    gather_rows(head, index_s, hs)
    row_sums(lambda at: weight[at, :] * hs[at, :], lhs, 0)
    sums = jnp.dot(lhs[...].astype(BF16), oh[...], preferred_element_type=F32)
    part[...] = jnp.zeros_like(part)
    part[0:1, :] = to_frame(sums[0:1] + sums[1:2] + sums[2:3])


def finish_last(ra, rb, band, head, rhs, inv, rim, reaches, out, section, one, two, spare, edge, mine, sems):
    sec = to_local(reaches[...])
    for t in range(2):
        mine[t : t + 1, :] = sec[:, REACH + t * 128 : REACH + (t + 1) * 128]
    moves = [
        pltpu.make_async_copy(
            head.at[tile_rows(c, 8, ROWS - 16), :], out.at[8 : ROWS - 8, c * 128 : (c + 1) * 128], sems.at[2 + c]
        )
        for c in range(TILES)
    ]
    moves.append(pltpu.make_async_copy(mine, section, sems.at[2 + TILES]))
    for m in moves:
        m.start()
    fill_spare(ra, rb, 1, 2, spare)
    done = band_relax(ra, rb, 2, band, halo_or_own(rhs, spare), halo_or_own(inv, rim), one, two)
    for c in range(TILES):
        at = slice(c * 128, (c + 1) * 128)
        edge[0, :, at] = head[tile_rows(c, 0, 8), :]
        edge[1, :, at] = head[tile_rows(c, ROWS - 8, 8), :]
        edge[0, 0:H, at] = done[0, c, 16 : 16 + H, :]
        edge[1, 8 - H : 8, at] = done[1, c, 16 - H : 16, :]
    edges = [
        pltpu.make_async_copy(edge.at[0], out.at[0:8, :], sems.at[0]),
        pltpu.make_async_copy(edge.at[1], out.at[ROWS - 8 : ROWS, :], sems.at[1]),
    ]
    for m in edges:
        m.start()
    for m in moves + edges:
        m.wait()


def shape(*dims, dtype=F32):
    return jax.ShapeDtypeStruct(dims, dtype)


def far(x):
    return pltpu.with_memory_space_constraint(x, pltpu.HBM)


def call(kernel, outs, ins, scratch=(), hbm=(), hbm_out=(), aliases=None, limit=16, flops=10_000_000):
    def at(k, far):
        return pl.BlockSpec(memory_space=pltpu.HBM if k in far else pltpu.VMEM)

    return pl.pallas_call(
        kernel,
        out_shape=outs,
        in_specs=[at(k, hbm) for k in range(len(ins))],
        out_specs=tuple(at(k, hbm_out) for k in range(len(outs))),
        scratch_shapes=list(scratch),
        input_output_aliases=aliases or {},
        compiler_params=pltpu.CompilerParams(vmem_limit_bytes=limit * 2**20),
        cost_estimate=pl.CostEstimate(flops=flops, bytes_accessed=4_000_000, transcendentals=0),
    )(*[far(x) if k in hbm else x for k, x in enumerate(ins)])


def swap(x, axis):
    return lax.ppermute(x, axis, [(k, k ^ 1) for k in range(lax.axis_size(axis))])


def far_swap(x, axis):
    n, m = lax.axis_size("row"), lax.axis_size("col")

    def partner(r, c):
        if axis == "col":
            return r, (c + 1) % m if c % 2 else (c - 1) % m
        if r in (0, n - 1):
            return r, c ^ 1
        return (r + 1 if r % 2 else r - 1), c

    pairs = []
    for r in range(n):
        for c in range(m):
            to = partner(r, c)
            pairs.append((r * m + c, to[0] * m + to[1]))
    return lax.ppermute(x, ("row", "col"), pairs)


def swap_both(a, b, axis):
    b = far_swap(b, axis)
    a = swap(a, axis)
    return a, b


def shift(x, axis, by):
    n = lax.axis_size(axis)
    return lax.ppermute(x, axis, [(k, (k + by) % n) for k in range(n)])


def exchange_sums(part):
    both = part + swap(part, "col")
    up = shift(both[:, 2 * REACH :], "col", 2)
    down = shift(both[:, : 2 * REACH], "col", -2)
    return both, up, down


EXT_SHAPE = shape(WIDE * EXT, 128)
GRID = shape(WIDE, ROWS, 128)
BAND = shape(2, WIDE, 8, 128)
SEG_ROWS = pltpu.VMEM((SEG, 128), F32)
SUMS = pltpu.VMEM((16, SEG), F32)
OTHER = pltpu.VMEM((WIDE * EXT, 128), F32)
WORK = pltpu.VMEM((2, WIDE, 32, 128), F32)
SPARE = pltpu.VMEM((2, WIDE, 8, 128), F32)
TURN = pltpu.VMEM((128, ROWS), F32)
SMALL = pltpu.SMEM((8, 128), I32)


def sems(n):
    return pltpu.SemaphoreType.DMA((n,))


def body(head0, recharge, storage, seg_block, seg_mask, seg_cond, seg_reach, bed, sec0, net, infl):
    part, oh, weight, head, index8 = call(
        prep,
        (shape(8, FRAME), shape(SEG, LOCAL, dtype=BF16), shape(SEG, 128), EXT_SHAPE, shape(8, 128, dtype=I32)),
        (
            head0,
            seg_block.reshape(8, 128),
            seg_reach.reshape(8, 128),
            seg_mask,
            seg_cond,
            bed.reshape(2, 128),
            sec0.reshape(2, 128),
            net.reshape(2, 128),
            infl,
        ),
        scratch=[
            SEG_ROWS,
            SUMS,
            pltpu.VMEM((8, 128), I32),
            pltpu.VMEM((8, 128), I32),
            pltpu.VMEM((SEG, 128), I32),
            SEG_ROWS,
            pltpu.VMEM((2, 128), F32),
            pltpu.VMEM((2, 128), F32),
            pltpu.VMEM((2, 128), I32),
            pltpu.SMEM((NETS,), F32),
            SMALL,
            sems(17),
        ],
        hbm=range(9),
    )
    own, up, down = exchange_sums(part)
    onehot, inv, supply = call(
        fields,
        (shape(TILES * ROWS, SEG, dtype=BF16), GRID, shape(TILES, ROWS, 128)),
        (head, recharge, storage, index8, weight),
        scratch=[pltpu.VMEM((ROWS, COLS), F32), pltpu.VMEM((ROWS, COLS), F32), sems(2)],
        hbm=(1, 2),
    )
    strip = shape(16, ROWS)
    pa, pb = call(functools.partial(columns, True), (strip, strip), (head, inv))
    mixed_shape = shape(SEG, 256, dtype=BF16)
    frame, mixed, rhs, ma, mb = call(
        functools.partial(section_kernel, True),
        (shape(8, FRAME), mixed_shape, GRID, strip, strip),
        (own, up, down, oh, onehot, weight, supply, pa, pb),
    )
    ca, cb = swap_both(ma, mb, "col")
    (rhs,) = call(inner_source, (GRID,), (onehot, mixed, supply, rhs), aliases={3: 0})
    rows = shape(96, 128)
    head, rhs, inv, sa, sb, band = call(
        functools.partial(place_columns, True),
        (EXT_SHAPE, GRID, GRID, rows, rows, BAND),
        (ca, cb, head, rhs, inv),
        scratch=[TURN],
        aliases={2: 0, 3: 1, 4: 2},
    )
    ra, rb = swap_both(sa, sb, "row")
    (head,) = call(inner_relax, (EXT_SHAPE,), (head, rhs, inv), scratch=[OTHER], aliases={0: 0})
    head, rim, part = call(
        finish_first,
        (EXT_SHAPE, BAND, shape(8, FRAME)),
        (ra, rb, band, head, rhs, inv, index8, weight, oh),
        scratch=[WORK, WORK, SEG_ROWS, SUMS, SPARE, SMALL, pltpu.SemaphoreType.DMA],
        aliases={3: 0},
    )
    own, up, down = exchange_sums(part)
    strip = shape(8, ROWS)
    pa, pb = call(functools.partial(columns, False), (strip, strip), (head,))
    reaches, mixed, rhs, ma, mb = call(
        functools.partial(section_kernel, False),
        (shape(1, FRAME), mixed_shape, GRID, strip, strip),
        (own, up, down, frame, oh, onehot, weight, supply, pa, pb),
    )
    ca, cb = swap_both(ma, mb, "col")
    (rhs,) = call(inner_source, (GRID,), (onehot, mixed, supply, rhs), aliases={3: 0})
    rows = shape(64, 128)
    head, rhs, sa, sb, band = call(
        functools.partial(place_columns, False),
        (EXT_SHAPE, GRID, rows, rows, BAND),
        (ca, cb, head, rhs),
        scratch=[TURN],
        aliases={2: 0, 3: 1},
    )
    ra, rb = swap_both(sa, sb, "row")
    (head,) = call(inner_relax, (EXT_SHAPE,), (head, rhs, inv), scratch=[OTHER], aliases={0: 0})
    out, section = call(
        finish_last,
        (shape(ROWS, COLS), shape(2, 128)),
        (ra, rb, band, head, rhs, inv, rim, reaches),
        scratch=[WORK, WORK, SPARE, pltpu.VMEM((2, 8, COLS), F32), pltpu.VMEM((2, 128), F32), sems(3 + TILES)],
        hbm_out=(0, 1),
    )
    return out, section.reshape(REACH)


def solution(mesh):
    placed = (
        P("row", "col"),
        P("row", "col"),
        P("row", "col"),
        P(("row", "col")),
        P(("row", "col"), None),
        P(("row", "col"), None),
        P(("row", "col")),
        P(("row", "col")),
        P(("row", "col")),
        P(("row", "col")),
        P(),
    )
    return jax.shard_map(
        body,
        mesh=mesh,
        in_specs=placed,
        out_specs=(P("row", "col"), P(("row", "col"))),
        check_vma=False,
    )
```

```python
import functools

import jax
import jax.numpy as jnp
from jax import lax
from jax.experimental import pallas as pl
from jax.experimental.pallas import tpu as pltpu
from jax.sharding import PartitionSpec as P

NETS = 64
SWEEPS = 4
ROWS, COLS = 384, 1024
TILES = COLS // 128
WIDE = TILES + 1
SEG = 1024
REACH = 256
FRAME = 4 * REACH
LOCAL = 3 * REACH
OFF = 8
EXT = ROWS + 2 * OFF
H = 4
DEPTH = (4, 3, 3)
UNROLL = 24
F32 = jnp.float32
BF16 = jnp.bfloat16
I32 = jnp.int32


def split2(x):
    hi = x.astype(BF16)
    lo = (x - hi.astype(F32)).astype(BF16)
    return hi, lo


def both_halves(x):
    return jnp.concatenate(split2(x), axis=1)


def column_of(row):
    return jnp.broadcast_to(row, (128, 128)).T


def tile_rows(c, start, size):
    return slice(c * EXT + OFF + start, c * EXT + OFF + start + size)


def gather_rows(head, index, out):
    def group(k, carry):
        for u in range(128):
            out[pl.ds(k * 128 + u, 1), :] = head[pl.ds(index[k, u], 1), :]
        return carry

    lax.fori_loop(0, SEG // 128, group, 0)


def row_sums(get, lhs, first):
    for k in range(SEG // 128):
        at = slice(k * 128, (k + 1) * 128)
        row = jnp.sum(get(at).T, axis=0, keepdims=True)
        hi = row.astype(BF16).astype(F32)
        mid = (row - hi).astype(BF16).astype(F32)
        lhs[first : first + 1, at] = hi
        lhs[first + 1 : first + 2, at] = mid
        lhs[first + 2 : first + 3, at] = row - hi - mid


def to_frame(row):
    odd = lax.axis_index("col") % 2 == 1
    parts = [row[:, m * REACH : (m + 1) * REACH] for m in range(3)]
    none = jnp.zeros_like(parts[0])
    pairs = zip([none] + parts, parts + [none])
    return jnp.concatenate([jnp.where(odd, a, b) for a, b in pairs], axis=1)


def to_local(row):
    odd = lax.axis_index("col") % 2 == 1
    parts = [row[:, m * REACH : (m + 1) * REACH] for m in range(4)]
    return jnp.concatenate([jnp.where(odd, b, a) for a, b in zip(parts[:3], parts[1:])], axis=1)


def prep(
    head, blk, reach, mask, condu, bed, sec0, net, infl, recharge,
    part, oh, weight, headx, index8, rech_v,
    hs, lhs, blk_v, reach_v, mask_v, cond_v, bed_v, sec0_v, net_v, infl_s, index_s, sems,
):
    moves = [
        pltpu.make_async_copy(blk, blk_v, sems.at[0]),
        pltpu.make_async_copy(reach, reach_v, sems.at[1]),
        pltpu.make_async_copy(mask, mask_v, sems.at[2]),
        pltpu.make_async_copy(condu, cond_v, sems.at[3]),
        pltpu.make_async_copy(bed, bed_v, sems.at[4]),
        pltpu.make_async_copy(sec0, sec0_v, sems.at[5]),
        pltpu.make_async_copy(net, net_v, sems.at[6]),
        pltpu.make_async_copy(infl, infl_s, sems.at[7]),
    ]
    heads = [
        pltpu.make_async_copy(
            head.at[:, c * 128 : (c + 1) * 128], headx.at[tile_rows(c, 0, ROWS), :], sems.at[8 + c]
        )
        for c in range(TILES)
    ]
    for m in moves + heads:
        m.start()
    j = lax.axis_index("col")
    base = j - 1
    for c in range(WIDE):
        headx[c * EXT : c * EXT + OFF, :] = jnp.zeros((OFF, 128), F32)
        headx[(c + 1) * EXT - OFF : (c + 1) * EXT, :] = jnp.zeros((OFF, 128), F32)
    headx[tile_rows(TILES, 0, ROWS), :] = jnp.zeros((ROWS, 128), F32)
    lhs[...] = jnp.zeros_like(lhs)
    part[...] = jnp.zeros_like(part)
    moves[0].wait()
    blocks = blk_v[...]
    index8[...] = (blocks & 7) * EXT + (blocks >> 3) + OFF
    listed = pltpu.make_async_copy(index8, index_s, sems.at[16])
    listed.start()
    moves[1].wait()
    reach8 = reach_v[...]
    slot8 = (((reach8 // REACH) % 16 - base + 16) % 16) * REACH + reach8 % REACH
    lane = lax.broadcasted_iota(I32, (128, 128), 1)
    for k in range(SEG // 128):
        slots = column_of(slot8[k : k + 1, :])
        for q in range(LOCAL // 128):
            oh[k * 128 : (k + 1) * 128, q * 128 : (q + 1) * 128] = jnp.where(
                slots == lane + q * 128, 1.0, 0.0
            ).astype(BF16)
    for m in moves[2:]:
        m.wait()
    nets = net_v[...]
    inflow = jnp.zeros(nets.shape, F32)
    for n in range(NETS):
        inflow = jnp.where(nets == n, infl_s[n], inflow)
    values = (bed_v[...], inflow, sec0_v[...])
    odd = j % 2
    for w in range(2):
        keep = odd == w
        for t in range(2):
            at = (1 + w) * REACH + t * 128
            for q, v in enumerate(values):
                part[2 + q : 3 + q, at : at + 128] = jnp.where(keep, v[t : t + 1, :], 0.0)
    weight[...] = mask_v[...].astype(F32) * cond_v[...]
    row_sums(lambda at: weight[at, :], lhs, 3)
    listed.wait()
    for m in heads:
        m.wait()
    later = pltpu.make_async_copy(recharge, rech_v, sems.at[17])
    later.start()
    gather_rows(headx, index_s, hs)
    row_sums(lambda at: weight[at, :] * hs[at, :], lhs, 0)
    sums = jnp.dot(lhs[...].astype(BF16), oh[...], preferred_element_type=F32)
    part[0:1, :] = to_frame(sums[0:1] + sums[1:2] + sums[2:3])
    part[1:2, :] = to_frame(sums[3:4] + sums[4:5] + sums[5:6])
    later.wait()


def one_hot(index8, storage, onehot, store_v, sem):
    move = pltpu.make_async_copy(storage, store_v, sem)
    move.start()
    target = index8[...]
    iota = lax.broadcasted_iota(I32, (ROWS, 128), 0)
    for k in range(SEG // 128):
        row = jnp.broadcast_to(target[k : k + 1, :], (ROWS, 128))
        for c in range(TILES):
            onehot[c * ROWS : (c + 1) * ROWS, k * 128 : (k + 1) * 128] = jnp.where(
                row == iota + (c * EXT + OFF), 1.0, 0.0
            ).astype(BF16)
    move.wait()


def fields(headx, rech_v, store_v, weight, onehot, inv, supply):
    both = both_halves(weight[...])
    inv[TILES] = jnp.zeros((ROWS, 128), F32)
    for c in range(TILES):
        at = slice(c * 128, (c + 1) * 128)
        got = jnp.dot(onehot[c * ROWS : (c + 1) * ROWS, :], both, preferred_element_type=F32)
        cond = got[:, :128] + got[:, 128:]
        store = store_v[:, at]
        inv[c] = 1.0 / (4.0 + store + cond)
        supply[c] = store * headx[tile_rows(c, 0, ROWS), :] + rech_v[:, at]


def put_columns(left_tile, right_tile, q, ma, mb):
    odd = lax.axis_index("col") % 2 == 1
    for k in range(ROWS // 128):
        at = slice(k * 128, (k + 1) * 128)
        left = left_tile(at).T[0:H, :]
        right = right_tile(at).T[128 - H : 128, :]
        ma[q * H : (q + 1) * H, at] = jnp.where(odd, left, right)
        mb[q * H : (q + 1) * H, at] = jnp.where(odd, right, left)


def columns(first, *refs):
    head = refs[0]
    ma, mb = refs[-2:]
    ma[...] = jnp.zeros_like(ma)
    mb[...] = jnp.zeros_like(mb)
    put_columns(
        lambda at: head[tile_rows(0, at.start, 128), :],
        lambda at: head[tile_rows(TILES - 1, at.start, 128), :],
        0, ma, mb,
    )
    if first:
        inv = refs[1]
        put_columns(lambda at: inv[0, at, :], lambda at: inv[TILES - 1, at, :], 2, ma, mb)


def section_kernel(first, *refs):
    if first:
        own, up, down, oh, onehot, weight, supply, pa, pb, frame, mixed, rhs, ma, mb = refs
    else:
        own, up, down, old, oh, onehot, weight, supply, pa, pb, reaches, mixed, rhs, ma, mb = refs
    full = own[...] + jnp.concatenate([up[...], down[...]], axis=1)
    leak = full[0:1]
    if first:
        wsum, bed, inflow, sec = full[1:2], full[2:3], full[3:4], full[4:5]
    else:
        wsum, bed, inflow, sec = (old[q : q + 1, :] for q in (1, 2, 3, 4))
    x = inflow - (sec * wsum - leak)
    soft = jnp.maximum(x, 0.0) + jnp.log1p(jnp.exp(-jnp.abs(x)))
    sec = bed + jnp.sqrt(1.0 + soft) - 1.0
    if first:
        frame[...] = full
        frame[4:5, :] = sec
    else:
        reaches[...] = sec
    hi, lo = split2(to_local(sec))
    wide = jnp.concatenate(
        [jnp.broadcast_to(hi.astype(F32), (128, LOCAL)), jnp.broadcast_to(lo.astype(F32), (128, LOCAL))], axis=0
    ).astype(BF16)
    got = lax.dot_general(oh[...], wide, (((1,), (1,)), ((), ())), preferred_element_type=F32)
    both = both_halves(weight[...] * (got[:, :128] + got[:, 128:]))
    mixed[...] = both
    ma[...] = pa[...]
    mb[...] = pb[...]
    for c in (0, TILES - 1):
        scatter(c, onehot, both, supply, rhs)
    put_columns(lambda at: rhs[0, at, :], lambda at: rhs[TILES - 1, at, :], 1, ma, mb)


def scatter(c, onehot, both, supply, rhs):
    got = jnp.dot(onehot[c * ROWS : (c + 1) * ROWS, :], both, preferred_element_type=F32)
    rhs[c] = supply[c] + got[:, :128] + got[:, 128:]


def inner_source(onehot, mixed, supply, rhs_in, rhs):
    both = mixed[...]
    for c in range(1, TILES - 1):
        scatter(c, onehot, both, supply, rhs)


def place_columns(first, *refs):
    if first:
        ca, cb, _, _, _, head, rhs, inv, sa, sb, band, wide = refs
        grids = (rhs, inv)
    else:
        ca, cb, _, _, head, rhs, sa, sb, band, wide = refs
        grids = (rhs,)
    i = lax.axis_index("row")
    j = lax.axis_index("col")
    odd = j % 2 == 1
    right = jnp.where(j == 15, 0.0, jnp.where(odd, cb[...], ca[...]))
    left = jnp.where(j == 0, 0.0, jnp.where(odd, ca[...], cb[...]))
    wide[...] = jnp.zeros_like(wide)
    row_odd = i % 2 == 1
    sa[...] = jnp.zeros_like(sa)
    sb[...] = jnp.zeros_like(sb)
    for q in range(1 + len(grids)):
        own = slice(q * H, (q + 1) * H)
        wide[0:H, :] = right[own, :]
        wide[128 - H : 128, :] = left[own, :]
        for k in range(ROWS // 128):
            turned = wide[:, k * 128 : (k + 1) * 128].T
            if q == 0:
                head[tile_rows(TILES, k * 128, 128), :] = turned
            else:
                grids[q - 1][TILES, k * 128 : (k + 1) * 128, :] = turned
        depth = DEPTH[q]
        for c in range(WIDE):
            if q == 0:
                top = head[tile_rows(c, 0, depth), :]
                bottom = head[tile_rows(c, ROWS - depth, depth), :]
            else:
                ref = grids[q - 1]
                top = ref[c, 0:depth, :]
                bottom = ref[c, ROWS - depth : ROWS, :]
            at = strip_rows(c, q, 1 + len(grids))
            sa[at, :] = jnp.where(row_odd, top, bottom)
            sb[at, :] = jnp.where(row_odd, bottom, top)
    for c in range(WIDE):
        band[0, c] = head[tile_rows(c, 0, 8), :]
        band[1, c] = head[tile_rows(c, ROWS - 8, 8), :]


def strip_rows(c, q, count):
    first = c * sum(DEPTH[:count]) + sum(DEPTH[:q])
    return slice(first, first + DEPTH[q])


def halo_rows(ra, rb, q, count, top, bottom):
    i = lax.axis_index("row")
    odd = i % 2 == 1
    for c in range(WIDE):
        at = strip_rows(c, q, count)
        a, b = ra[at, :], rb[at, :]
        top(c, jnp.where(i == 0, 0.0, jnp.where(odd, a, b)))
        bottom(c, jnp.where(i == 15, 0.0, jnp.where(odd, b, a)))


def relax_chunk(src, dst, rhs, inv, spread):
    lane = lax.broadcasted_iota(I32, (8, 128), 1)
    mid = [src(c, 0) for c in range(WIDE)]
    fwd = [pltpu.roll(m, 1, 1) for m in mid]
    bwd = [pltpu.roll(m, 127, 1) for m in mid]
    for c in range(spread):
        left = jnp.where(lane == 0, fwd[c - 1], fwd[c])
        right = jnp.where(lane == 127, bwd[(c + 1) % WIDE], bwd[c])
        total = (src(c, -1) + src(c, 1)) + (left + right) + rhs(c)
        dst(c, total * inv(c))


def sweep(src, dst, rhs, inv):
    def put(c, r, value):
        dst[pl.ds(c * EXT + OFF + r, 8), :] = value

    def group(g, carry):
        for u in range(UNROLL):
            r = g * (8 * UNROLL) + u * 8
            relax_chunk(
                lambda c, d: src[pl.ds(c * EXT + OFF + r + d, 8), :],
                lambda c, value: put(c, r, value),
                lambda c: rhs[c, pl.ds(r, 8), :],
                lambda c: inv[c, pl.ds(r, 8), :],
                WIDE,
            )
        return carry

    lax.fori_loop(0, ROWS // (8 * UNROLL), group, 0)


def sweeps(head, other, rhs, inv):
    for c in range(WIDE):
        other[c * EXT : c * EXT + OFF, :] = jnp.zeros((OFF, 128), F32)
        other[(c + 1) * EXT - OFF : (c + 1) * EXT, :] = jnp.zeros((OFF, 128), F32)
    for _ in range(SWEEPS // 2):
        sweep(head, other, rhs, inv)
        sweep(other, head, rhs, inv)


def inner_relax(head_in, rhs, inv, head, other):
    sweeps(head, other, rhs, inv)


def band_relax(ra, rb, count, band, get_rhs, get_inv, one, two):
    one[...] = jnp.zeros_like(one)
    two[...] = jnp.zeros_like(two)
    for c in range(WIDE):
        one[0, c, 16:24, :] = band[0, c]
        one[1, c, 8:16, :] = band[1, c]

    def top(c, value):
        one[0, c, 16 - H : 16, :] = value

    def bottom(c, value):
        one[1, c, 16 : 16 + H, :] = value

    halo_rows(ra, rb, 0, count, top, bottom)
    src, dst = one, two
    for _ in range(SWEEPS):
        for side in range(2):
            for t in range(2):
                r = 8 + t * 8

                def put(c, value):
                    dst[side, c, r : r + 8, :] = value

                relax_chunk(
                    lambda c, d: src[side, c, r + d : r + d + 8, :],
                    put,
                    lambda c: get_rhs(side, c, t),
                    lambda c: get_inv(side, c, t),
                    WIDE,
                )
        src, dst = dst, src
    return one


def halo_or_own(ref, spare):
    def get(side, c, t):
        if side == 0:
            return ref[c, 0:8, :] if t == 1 else spare[0, c]
        return ref[c, ROWS - 8 : ROWS, :] if t == 0 else spare[1, c]

    return get


def fill_spare(ra, rb, q, count, spare):
    spare[...] = jnp.zeros_like(spare)

    def top(c, value):
        spare[0, c, 8 - DEPTH[q] : 8, :] = value

    def bottom(c, value):
        spare[1, c, 0 : DEPTH[q], :] = value

    halo_rows(ra, rb, q, count, top, bottom)


def finish_first(
    ra, rb, band, head_in, rhs, inv, index8, weight, oh, head, rim, part, one, two, hs, lhs, spare, index_s, sem
):
    listed = pltpu.make_async_copy(index8, index_s, sem)
    listed.start()
    fill_spare(ra, rb, 1, 3, spare)
    fill_spare(ra, rb, 2, 3, rim)
    done = band_relax(ra, rb, 3, band, halo_or_own(rhs, spare), halo_or_own(inv, rim), one, two)
    for c in range(TILES):
        head[tile_rows(c, 0, H), :] = done[0, c, 16 : 16 + H, :]
        head[tile_rows(c, ROWS - H, H), :] = done[1, c, 16 - H : 16, :]
    listed.wait()
    lhs[...] = jnp.zeros_like(lhs)
    gather_rows(head, index_s, hs)
    row_sums(lambda at: weight[at, :] * hs[at, :], lhs, 0)
    sums = jnp.dot(lhs[...].astype(BF16), oh[...], preferred_element_type=F32)
    part[...] = jnp.zeros_like(part)
    part[0:1, :] = to_frame(sums[0:1] + sums[1:2] + sums[2:3])


def finish_last(ra, rb, band, head, rhs, inv, rim, reaches, out, section, one, two, spare, edge, mine, sems):
    sec = to_local(reaches[...])
    for t in range(2):
        mine[t : t + 1, :] = sec[:, REACH + t * 128 : REACH + (t + 1) * 128]
    moves = [
        pltpu.make_async_copy(
            head.at[tile_rows(c, 8, ROWS - 16), :], out.at[8 : ROWS - 8, c * 128 : (c + 1) * 128], sems.at[2 + c]
        )
        for c in range(TILES)
    ]
    moves.append(pltpu.make_async_copy(mine, section, sems.at[2 + TILES]))
    for m in moves:
        m.start()
    fill_spare(ra, rb, 1, 2, spare)
    done = band_relax(ra, rb, 2, band, halo_or_own(rhs, spare), halo_or_own(inv, rim), one, two)
    for c in range(TILES):
        at = slice(c * 128, (c + 1) * 128)
        edge[0, :, at] = head[tile_rows(c, 0, 8), :]
        edge[1, :, at] = head[tile_rows(c, ROWS - 8, 8), :]
        edge[0, 0:H, at] = done[0, c, 16 : 16 + H, :]
        edge[1, 8 - H : 8, at] = done[1, c, 16 - H : 16, :]
    edges = [
        pltpu.make_async_copy(edge.at[0], out.at[0:8, :], sems.at[0]),
        pltpu.make_async_copy(edge.at[1], out.at[ROWS - 8 : ROWS, :], sems.at[1]),
    ]
    for m in edges:
        m.start()
    for m in moves + edges:
        m.wait()


def shape(*dims, dtype=F32):
    return jax.ShapeDtypeStruct(dims, dtype)


def far(x):
    return pltpu.with_memory_space_constraint(x, pltpu.HBM)


def call(kernel, outs, ins, scratch=(), hbm=(), hbm_out=(), aliases=None, limit=16, flops=10_000_000):
    def at(k, far):
        return pl.BlockSpec(memory_space=pltpu.HBM if k in far else pltpu.VMEM)

    return pl.pallas_call(
        kernel,
        out_shape=outs,
        in_specs=[at(k, hbm) for k in range(len(ins))],
        out_specs=tuple(at(k, hbm_out) for k in range(len(outs))),
        scratch_shapes=list(scratch),
        input_output_aliases=aliases or {},
        compiler_params=pltpu.CompilerParams(vmem_limit_bytes=limit * 2**20),
        cost_estimate=pl.CostEstimate(flops=flops, bytes_accessed=4_000_000, transcendentals=0),
    )(*[far(x) if k in hbm else x for k, x in enumerate(ins)])


def swap(x, axis):
    return lax.ppermute(x, axis, [(k, k ^ 1) for k in range(lax.axis_size(axis))])


def far_swap(x, axis):
    n, m = lax.axis_size("row"), lax.axis_size("col")

    def partner(r, c):
        if axis == "col":
            return r, (c + 1) % m if c % 2 else (c - 1) % m
        if r in (0, n - 1):
            return r, c ^ 1
        return (r + 1 if r % 2 else r - 1), c

    pairs = []
    for r in range(n):
        for c in range(m):
            to = partner(r, c)
            pairs.append((r * m + c, to[0] * m + to[1]))
    return lax.ppermute(x, ("row", "col"), pairs)


def swap_both(a, b, axis):
    b = far_swap(b, axis)
    a = swap(a, axis)
    return a, b


def shift(x, axis, by):
    n = lax.axis_size(axis)
    return lax.ppermute(x, axis, [(k, (k + by) % n) for k in range(n)])


def exchange_sums(part):
    both = part + swap(part, "col")
    up = shift(both[:, 2 * REACH :], "col", 2)
    down = shift(both[:, : 2 * REACH], "col", -2)
    return both, up, down


EXT_SHAPE = shape(WIDE * EXT, 128)
GRID = shape(WIDE, ROWS, 128)
BAND = shape(2, WIDE, 8, 128)
SEG_ROWS = pltpu.VMEM((SEG, 128), F32)
SUMS = pltpu.VMEM((16, SEG), F32)
OTHER = pltpu.VMEM((WIDE * EXT, 128), F32)
WORK = pltpu.VMEM((2, WIDE, 32, 128), F32)
SPARE = pltpu.VMEM((2, WIDE, 8, 128), F32)
TURN = pltpu.VMEM((128, ROWS), F32)
SMALL = pltpu.SMEM((8, 128), I32)


def sems(n):
    return pltpu.SemaphoreType.DMA((n,))


def body(head0, recharge, storage, seg_block, seg_mask, seg_cond, seg_reach, bed, sec0, net, infl):
    part, oh, weight, head, index8, rech = call(
        prep,
        (shape(8, FRAME), shape(SEG, LOCAL, dtype=BF16), shape(SEG, 128), EXT_SHAPE, shape(8, 128, dtype=I32), shape(ROWS, COLS)),
        (
            head0,
            seg_block.reshape(8, 128),
            seg_reach.reshape(8, 128),
            seg_mask,
            seg_cond,
            bed.reshape(2, 128),
            sec0.reshape(2, 128),
            net.reshape(2, 128),
            infl,
            recharge,
        ),
        scratch=[
            SEG_ROWS,
            SUMS,
            pltpu.VMEM((8, 128), I32),
            pltpu.VMEM((8, 128), I32),
            pltpu.VMEM((SEG, 128), I32),
            SEG_ROWS,
            pltpu.VMEM((2, 128), F32),
            pltpu.VMEM((2, 128), F32),
            pltpu.VMEM((2, 128), I32),
            pltpu.SMEM((NETS,), F32),
            SMALL,
            sems(18),
        ],
        hbm=range(10),
    )
    own, up, down = exchange_sums(part)
    onehot, store = call(
        one_hot,
        (shape(TILES * ROWS, SEG, dtype=BF16), shape(ROWS, COLS)),
        (index8, storage),
        scratch=[pltpu.SemaphoreType.DMA],
        hbm=(1,),
    )
    inv, supply = call(fields, (GRID, shape(TILES, ROWS, 128)), (head, rech, store, weight, onehot))
    strip = shape(16, ROWS)
    pa, pb = call(functools.partial(columns, True), (strip, strip), (head, inv))
    mixed_shape = shape(SEG, 256, dtype=BF16)
    frame, mixed, rhs, ma, mb = call(
        functools.partial(section_kernel, True),
        (shape(8, FRAME), mixed_shape, GRID, strip, strip),
        (own, up, down, oh, onehot, weight, supply, pa, pb),
    )
    ca, cb = swap_both(ma, mb, "col")
    (rhs,) = call(inner_source, (GRID,), (onehot, mixed, supply, rhs), aliases={3: 0})
    rows = shape(96, 128)
    head, rhs, inv, sa, sb, band = call(
        functools.partial(place_columns, True),
        (EXT_SHAPE, GRID, GRID, rows, rows, BAND),
        (ca, cb, head, rhs, inv),
        scratch=[TURN],
        aliases={2: 0, 3: 1, 4: 2},
    )
    ra, rb = swap_both(sa, sb, "row")
    (head,) = call(inner_relax, (EXT_SHAPE,), (head, rhs, inv), scratch=[OTHER], aliases={0: 0})
    head, rim, part = call(
        finish_first,
        (EXT_SHAPE, BAND, shape(8, FRAME)),
        (ra, rb, band, head, rhs, inv, index8, weight, oh),
        scratch=[WORK, WORK, SEG_ROWS, SUMS, SPARE, SMALL, pltpu.SemaphoreType.DMA],
        aliases={3: 0},
    )
    own, up, down = exchange_sums(part)
    strip = shape(8, ROWS)
    pa, pb = call(functools.partial(columns, False), (strip, strip), (head,))
    reaches, mixed, rhs, ma, mb = call(
        functools.partial(section_kernel, False),
        (shape(1, FRAME), mixed_shape, GRID, strip, strip),
        (own, up, down, frame, oh, onehot, weight, supply, pa, pb),
    )
    ca, cb = swap_both(ma, mb, "col")
    (rhs,) = call(inner_source, (GRID,), (onehot, mixed, supply, rhs), aliases={3: 0})
    rows = shape(64, 128)
    head, rhs, sa, sb, band = call(
        functools.partial(place_columns, False),
        (EXT_SHAPE, GRID, rows, rows, BAND),
        (ca, cb, head, rhs),
        scratch=[TURN],
        aliases={2: 0, 3: 1},
    )
    ra, rb = swap_both(sa, sb, "row")
    (head,) = call(inner_relax, (EXT_SHAPE,), (head, rhs, inv), scratch=[OTHER], aliases={0: 0})
    out, section = call(
        finish_last,
        (shape(ROWS, COLS), shape(2, 128)),
        (ra, rb, band, head, rhs, inv, rim, reaches),
        scratch=[WORK, WORK, SPARE, pltpu.VMEM((2, 8, COLS), F32), pltpu.VMEM((2, 128), F32), sems(3 + TILES)],
        hbm_out=(0, 1),
    )
    return out, section.reshape(REACH)


def solution(mesh):
    placed = (
        P("row", "col"),
        P("row", "col"),
        P("row", "col"),
        P(("row", "col")),
        P(("row", "col"), None),
        P(("row", "col"), None),
        P(("row", "col")),
        P(("row", "col")),
        P(("row", "col")),
        P(("row", "col")),
        P(),
    )
    return jax.shard_map(
        body,
        mesh=mesh,
        in_specs=placed,
        out_specs=(P("row", "col"), P(("row", "col"))),
        check_vma=False,
    )
```

```python
import functools

import jax
import jax.numpy as jnp
from jax import lax
from jax.experimental import pallas as pl
from jax.experimental.pallas import tpu as pltpu
from jax.sharding import PartitionSpec as P

NETS = 64
SWEEPS = 4
ROWS, COLS = 384, 1024
TILES = COLS // 128
WIDE = TILES + 1
SEG = 1024
REACH = 256
FRAME = 4 * REACH
LOCAL = 3 * REACH
OFF = 8
EXT = ROWS + 2 * OFF
H = 4
DEPTH = (4, 3, 3)
UNROLL = 48
F32 = jnp.float32
BF16 = jnp.bfloat16
I32 = jnp.int32


def split2(x):
    hi = x.astype(BF16)
    lo = (x - hi.astype(F32)).astype(BF16)
    return hi, lo


def both_halves(x):
    return jnp.concatenate(split2(x), axis=1)


def column_of(row):
    return jnp.broadcast_to(row, (128, 128)).T


def tile_rows(c, start, size):
    return slice(c * EXT + OFF + start, c * EXT + OFF + start + size)


def gather_rows(head, index, out):
    def group(k, carry):
        for u in range(128):
            out[pl.ds(k * 128 + u, 1), :] = head[pl.ds(index[k, u], 1), :]
        return carry

    lax.fori_loop(0, SEG // 128, group, 0)


def row_sums(get, lhs, first):
    for k in range(SEG // 128):
        at = slice(k * 128, (k + 1) * 128)
        row = jnp.sum(get(at).T, axis=0, keepdims=True)
        hi = row.astype(BF16).astype(F32)
        mid = (row - hi).astype(BF16).astype(F32)
        lhs[first : first + 1, at] = hi
        lhs[first + 1 : first + 2, at] = mid
        lhs[first + 2 : first + 3, at] = row - hi - mid


def to_frame(row):
    odd = lax.axis_index("col") % 2 == 1
    parts = [row[:, m * REACH : (m + 1) * REACH] for m in range(3)]
    none = jnp.zeros_like(parts[0])
    pairs = zip([none] + parts, parts + [none])
    return jnp.concatenate([jnp.where(odd, a, b) for a, b in pairs], axis=1)


def to_local(row):
    odd = lax.axis_index("col") % 2 == 1
    parts = [row[:, m * REACH : (m + 1) * REACH] for m in range(4)]
    return jnp.concatenate([jnp.where(odd, b, a) for a, b in zip(parts[:3], parts[1:])], axis=1)


def prep(
    head, blk, reach, mask, condu, bed, sec0, net, infl, recharge,
    part, oh, weight, headx, index8, rech_v,
    hs, lhs, blk_v, reach_v, mask_v, cond_v, bed_v, sec0_v, net_v, infl_s, index_s, sems,
):
    moves = [
        pltpu.make_async_copy(blk, blk_v, sems.at[0]),
        pltpu.make_async_copy(reach, reach_v, sems.at[1]),
        pltpu.make_async_copy(mask, mask_v, sems.at[2]),
        pltpu.make_async_copy(condu, cond_v, sems.at[3]),
        pltpu.make_async_copy(bed, bed_v, sems.at[4]),
        pltpu.make_async_copy(sec0, sec0_v, sems.at[5]),
        pltpu.make_async_copy(net, net_v, sems.at[6]),
        pltpu.make_async_copy(infl, infl_s, sems.at[7]),
    ]
    heads = [
        pltpu.make_async_copy(
            head.at[:, c * 128 : (c + 1) * 128], headx.at[tile_rows(c, 0, ROWS), :], sems.at[8 + c]
        )
        for c in range(TILES)
    ]
    for m in moves + heads:
        m.start()
    j = lax.axis_index("col")
    base = j - 1
    for c in range(WIDE):
        headx[c * EXT : c * EXT + OFF, :] = jnp.zeros((OFF, 128), F32)
        headx[(c + 1) * EXT - OFF : (c + 1) * EXT, :] = jnp.zeros((OFF, 128), F32)
    headx[tile_rows(TILES, 0, ROWS), :] = jnp.zeros((ROWS, 128), F32)
    lhs[...] = jnp.zeros_like(lhs)
    part[...] = jnp.zeros_like(part)
    moves[0].wait()
    blocks = blk_v[...]
    index8[...] = (blocks & 7) * EXT + (blocks >> 3) + OFF
    listed = pltpu.make_async_copy(index8, index_s, sems.at[16])
    listed.start()
    moves[1].wait()
    reach8 = reach_v[...]
    slot8 = (((reach8 // REACH) % 16 - base + 16) % 16) * REACH + reach8 % REACH
    lane = lax.broadcasted_iota(I32, (128, 128), 1)
    for k in range(SEG // 128):
        slots = column_of(slot8[k : k + 1, :])
        for q in range(LOCAL // 128):
            oh[k * 128 : (k + 1) * 128, q * 128 : (q + 1) * 128] = jnp.where(
                slots == lane + q * 128, 1.0, 0.0
            ).astype(BF16)
    for m in moves[2:]:
        m.wait()
    nets = net_v[...]
    inflow = jnp.zeros(nets.shape, F32)
    for n in range(NETS):
        inflow = jnp.where(nets == n, infl_s[n], inflow)
    values = (bed_v[...], inflow, sec0_v[...])
    odd = j % 2
    for w in range(2):
        keep = odd == w
        for t in range(2):
            at = (1 + w) * REACH + t * 128
            for q, v in enumerate(values):
                part[2 + q : 3 + q, at : at + 128] = jnp.where(keep, v[t : t + 1, :], 0.0)
    weight[...] = mask_v[...].astype(F32) * cond_v[...]
    row_sums(lambda at: weight[at, :], lhs, 3)
    listed.wait()
    for m in heads:
        m.wait()
    later = pltpu.make_async_copy(recharge, rech_v, sems.at[17])
    later.start()
    gather_rows(headx, index_s, hs)
    row_sums(lambda at: weight[at, :] * hs[at, :], lhs, 0)
    sums = jnp.dot(lhs[...].astype(BF16), oh[...], preferred_element_type=F32)
    part[0:1, :] = to_frame(sums[0:1] + sums[1:2] + sums[2:3])
    part[1:2, :] = to_frame(sums[3:4] + sums[4:5] + sums[5:6])
    later.wait()


def one_hot(index8, onehot):
    target = index8[...]
    iota = lax.broadcasted_iota(I32, (ROWS, 128), 0)
    for k in range(SEG // 128):
        row = jnp.broadcast_to(target[k : k + 1, :], (ROWS, 128))
        for c in range(TILES):
            onehot[c * ROWS : (c + 1) * ROWS, k * 128 : (k + 1) * 128] = jnp.where(
                row == iota + (c * EXT + OFF), 1.0, 0.0
            ).astype(BF16)


def fields(headx, rech_v, store_v, weight, onehot, inv, supply):
    both = both_halves(weight[...])
    inv[TILES] = jnp.zeros((ROWS, 128), F32)
    for c in range(TILES):
        at = slice(c * 128, (c + 1) * 128)
        got = jnp.dot(onehot[c * ROWS : (c + 1) * ROWS, :], both, preferred_element_type=F32)
        cond = got[:, :128] + got[:, 128:]
        store = store_v[:, at]
        inv[c] = 1.0 / (4.0 + store + cond)
        supply[c] = store * headx[tile_rows(c, 0, ROWS), :] + rech_v[:, at]


def put_columns(left_tile, right_tile, q, ma, mb):
    odd = lax.axis_index("col") % 2 == 1
    for k in range(ROWS // 128):
        at = slice(k * 128, (k + 1) * 128)
        left = left_tile(at).T[0:H, :]
        right = right_tile(at).T[128 - H : 128, :]
        ma[q * H : (q + 1) * H, at] = jnp.where(odd, left, right)
        mb[q * H : (q + 1) * H, at] = jnp.where(odd, right, left)


def columns(first, *refs):
    head = refs[0]
    ma, mb = refs[-2:]
    ma[...] = jnp.zeros_like(ma)
    mb[...] = jnp.zeros_like(mb)
    put_columns(
        lambda at: head[tile_rows(0, at.start, 128), :],
        lambda at: head[tile_rows(TILES - 1, at.start, 128), :],
        0, ma, mb,
    )
    if first:
        inv = refs[1]
        put_columns(lambda at: inv[0, at, :], lambda at: inv[TILES - 1, at, :], 2, ma, mb)


def section_kernel(first, *refs):
    if first:
        own, up, down, oh, onehot, weight, supply, pa, pb, frame, mixed, rhs, ma, mb = refs
    else:
        own, up, down, old, oh, onehot, weight, supply, pa, pb, reaches, mixed, rhs, ma, mb = refs
    full = own[...] + jnp.concatenate([up[...], down[...]], axis=1)
    leak = full[0:1]
    if first:
        wsum, bed, inflow, sec = full[1:2], full[2:3], full[3:4], full[4:5]
    else:
        wsum, bed, inflow, sec = (old[q : q + 1, :] for q in (1, 2, 3, 4))
    x = inflow - (sec * wsum - leak)
    soft = jnp.maximum(x, 0.0) + jnp.log1p(jnp.exp(-jnp.abs(x)))
    sec = bed + jnp.sqrt(1.0 + soft) - 1.0
    if first:
        frame[...] = full
        frame[4:5, :] = sec
    else:
        reaches[...] = sec
    hi, lo = split2(to_local(sec))
    wide = jnp.concatenate(
        [jnp.broadcast_to(hi.astype(F32), (128, LOCAL)), jnp.broadcast_to(lo.astype(F32), (128, LOCAL))], axis=0
    ).astype(BF16)
    got = lax.dot_general(oh[...], wide, (((1,), (1,)), ((), ())), preferred_element_type=F32)
    both = both_halves(weight[...] * (got[:, :128] + got[:, 128:]))
    mixed[...] = both
    ma[...] = pa[...]
    mb[...] = pb[...]
    for c in (0, TILES - 1):
        scatter(c, onehot, both, supply, rhs)
    put_columns(lambda at: rhs[0, at, :], lambda at: rhs[TILES - 1, at, :], 1, ma, mb)


def scatter(c, onehot, both, supply, rhs):
    got = jnp.dot(onehot[c * ROWS : (c + 1) * ROWS, :], both, preferred_element_type=F32)
    rhs[c] = supply[c] + got[:, :128] + got[:, 128:]


def inner_source(onehot, mixed, supply, rhs_in, rhs):
    both = mixed[...]
    for c in range(1, TILES - 1):
        scatter(c, onehot, both, supply, rhs)


def place_columns(first, *refs):
    if first:
        ca, cb, _, _, _, head, rhs, inv, sa, sb, band, wide = refs
        grids = (rhs, inv)
    else:
        ca, cb, _, _, head, rhs, sa, sb, band, wide = refs
        grids = (rhs,)
    i = lax.axis_index("row")
    j = lax.axis_index("col")
    odd = j % 2 == 1
    right = jnp.where(j == 15, 0.0, jnp.where(odd, cb[...], ca[...]))
    left = jnp.where(j == 0, 0.0, jnp.where(odd, ca[...], cb[...]))
    wide[...] = jnp.zeros_like(wide)
    row_odd = i % 2 == 1
    sa[...] = jnp.zeros_like(sa)
    sb[...] = jnp.zeros_like(sb)
    for q in range(1 + len(grids)):
        own = slice(q * H, (q + 1) * H)
        wide[0:H, :] = right[own, :]
        wide[128 - H : 128, :] = left[own, :]
        for k in range(ROWS // 128):
            turned = wide[:, k * 128 : (k + 1) * 128].T
            if q == 0:
                head[tile_rows(TILES, k * 128, 128), :] = turned
            else:
                grids[q - 1][TILES, k * 128 : (k + 1) * 128, :] = turned
        depth = DEPTH[q]
        for c in range(WIDE):
            if q == 0:
                top = head[tile_rows(c, 0, depth), :]
                bottom = head[tile_rows(c, ROWS - depth, depth), :]
            else:
                ref = grids[q - 1]
                top = ref[c, 0:depth, :]
                bottom = ref[c, ROWS - depth : ROWS, :]
            at = strip_rows(c, q, 1 + len(grids))
            sa[at, :] = jnp.where(row_odd, top, bottom)
            sb[at, :] = jnp.where(row_odd, bottom, top)
    for c in range(WIDE):
        band[0, c] = head[tile_rows(c, 0, 8), :]
        band[1, c] = head[tile_rows(c, ROWS - 8, 8), :]


def strip_rows(c, q, count):
    first = c * sum(DEPTH[:count]) + sum(DEPTH[:q])
    return slice(first, first + DEPTH[q])


def halo_rows(ra, rb, q, count, top, bottom):
    i = lax.axis_index("row")
    odd = i % 2 == 1
    for c in range(WIDE):
        at = strip_rows(c, q, count)
        a, b = ra[at, :], rb[at, :]
        top(c, jnp.where(i == 0, 0.0, jnp.where(odd, a, b)))
        bottom(c, jnp.where(i == 15, 0.0, jnp.where(odd, b, a)))


def relax_chunk(src, dst, rhs, inv, spread):
    lane = lax.broadcasted_iota(I32, (8, 128), 1)
    mid = [src(c, 0) for c in range(WIDE)]
    fwd = [pltpu.roll(m, 1, 1) for m in mid]
    bwd = [pltpu.roll(m, 127, 1) for m in mid]
    for c in range(spread):
        left = jnp.where(lane == 0, fwd[c - 1], fwd[c])
        right = jnp.where(lane == 127, bwd[(c + 1) % WIDE], bwd[c])
        total = (src(c, -1) + src(c, 1)) + (left + right) + rhs(c)
        dst(c, total * inv(c))


def sweep(src, dst, rhs, inv):
    def put(c, r, value):
        dst[pl.ds(c * EXT + OFF + r, 8), :] = value

    def group(g, carry):
        for u in range(UNROLL):
            r = g * (8 * UNROLL) + u * 8
            relax_chunk(
                lambda c, d: src[pl.ds(c * EXT + OFF + r + d, 8), :],
                lambda c, value: put(c, r, value),
                lambda c: rhs[c, pl.ds(r, 8), :],
                lambda c: inv[c, pl.ds(r, 8), :],
                WIDE,
            )
        return carry

    lax.fori_loop(0, ROWS // (8 * UNROLL), group, 0)


def sweeps(head, other, rhs, inv):
    for c in range(WIDE):
        other[c * EXT : c * EXT + OFF, :] = jnp.zeros((OFF, 128), F32)
        other[(c + 1) * EXT - OFF : (c + 1) * EXT, :] = jnp.zeros((OFF, 128), F32)
    for _ in range(SWEEPS // 2):
        sweep(head, other, rhs, inv)
        sweep(other, head, rhs, inv)


def inner_relax(head_in, rhs, inv, head, other):
    sweeps(head, other, rhs, inv)


def band_relax(ra, rb, count, band, get_rhs, get_inv, one, two):
    one[...] = jnp.zeros_like(one)
    two[...] = jnp.zeros_like(two)
    for c in range(WIDE):
        one[0, c, 16:24, :] = band[0, c]
        one[1, c, 8:16, :] = band[1, c]

    def top(c, value):
        one[0, c, 16 - H : 16, :] = value

    def bottom(c, value):
        one[1, c, 16 : 16 + H, :] = value

    halo_rows(ra, rb, 0, count, top, bottom)
    src, dst = one, two
    for _ in range(SWEEPS):
        for side in range(2):
            for t in range(2):
                r = 8 + t * 8

                def put(c, value):
                    dst[side, c, r : r + 8, :] = value

                relax_chunk(
                    lambda c, d: src[side, c, r + d : r + d + 8, :],
                    put,
                    lambda c: get_rhs(side, c, t),
                    lambda c: get_inv(side, c, t),
                    WIDE,
                )
        src, dst = dst, src
    return one


def halo_or_own(ref, spare):
    def get(side, c, t):
        if side == 0:
            return ref[c, 0:8, :] if t == 1 else spare[0, c]
        return ref[c, ROWS - 8 : ROWS, :] if t == 0 else spare[1, c]

    return get


def fill_spare(ra, rb, q, count, spare):
    spare[...] = jnp.zeros_like(spare)

    def top(c, value):
        spare[0, c, 8 - DEPTH[q] : 8, :] = value

    def bottom(c, value):
        spare[1, c, 0 : DEPTH[q], :] = value

    halo_rows(ra, rb, q, count, top, bottom)


def finish_first(
    ra, rb, band, head_in, rhs, inv, index8, weight, oh, head, rim, part, one, two, hs, lhs, spare, index_s, sem
):
    listed = pltpu.make_async_copy(index8, index_s, sem)
    listed.start()
    fill_spare(ra, rb, 1, 3, spare)
    fill_spare(ra, rb, 2, 3, rim)
    done = band_relax(ra, rb, 3, band, halo_or_own(rhs, spare), halo_or_own(inv, rim), one, two)
    for c in range(TILES):
        head[tile_rows(c, 0, H), :] = done[0, c, 16 : 16 + H, :]
        head[tile_rows(c, ROWS - H, H), :] = done[1, c, 16 - H : 16, :]
    listed.wait()
    lhs[...] = jnp.zeros_like(lhs)
    gather_rows(head, index_s, hs)
    row_sums(lambda at: weight[at, :] * hs[at, :], lhs, 0)
    sums = jnp.dot(lhs[...].astype(BF16), oh[...], preferred_element_type=F32)
    part[...] = jnp.zeros_like(part)
    part[0:1, :] = to_frame(sums[0:1] + sums[1:2] + sums[2:3])


def finish_last(ra, rb, band, head, rhs, inv, rim, reaches, out, section, one, two, spare, edge, mine, sems):
    sec = to_local(reaches[...])
    for t in range(2):
        mine[t : t + 1, :] = sec[:, REACH + t * 128 : REACH + (t + 1) * 128]
    moves = [
        pltpu.make_async_copy(
            head.at[tile_rows(c, 8, ROWS - 16), :], out.at[8 : ROWS - 8, c * 128 : (c + 1) * 128], sems.at[2 + c]
        )
        for c in range(TILES)
    ]
    moves.append(pltpu.make_async_copy(mine, section, sems.at[2 + TILES]))
    for m in moves:
        m.start()
    fill_spare(ra, rb, 1, 2, spare)
    done = band_relax(ra, rb, 2, band, halo_or_own(rhs, spare), halo_or_own(inv, rim), one, two)
    for c in range(TILES):
        at = slice(c * 128, (c + 1) * 128)
        edge[0, :, at] = head[tile_rows(c, 0, 8), :]
        edge[1, :, at] = head[tile_rows(c, ROWS - 8, 8), :]
        edge[0, 0:H, at] = done[0, c, 16 : 16 + H, :]
        edge[1, 8 - H : 8, at] = done[1, c, 16 - H : 16, :]
    edges = [
        pltpu.make_async_copy(edge.at[0], out.at[0:8, :], sems.at[0]),
        pltpu.make_async_copy(edge.at[1], out.at[ROWS - 8 : ROWS, :], sems.at[1]),
    ]
    for m in edges:
        m.start()
    for m in moves + edges:
        m.wait()


def shape(*dims, dtype=F32):
    return jax.ShapeDtypeStruct(dims, dtype)


def far(x):
    return pltpu.with_memory_space_constraint(x, pltpu.HBM)


def call(kernel, outs, ins, scratch=(), hbm=(), hbm_out=(), aliases=None, limit=16, flops=10_000_000):
    def at(k, far):
        return pl.BlockSpec(memory_space=pltpu.HBM if k in far else pltpu.VMEM)

    return pl.pallas_call(
        kernel,
        out_shape=outs,
        in_specs=[at(k, hbm) for k in range(len(ins))],
        out_specs=tuple(at(k, hbm_out) for k in range(len(outs))),
        scratch_shapes=list(scratch),
        input_output_aliases=aliases or {},
        compiler_params=pltpu.CompilerParams(vmem_limit_bytes=limit * 2**20),
        cost_estimate=pl.CostEstimate(flops=flops, bytes_accessed=4_000_000, transcendentals=0),
    )(*[far(x) if k in hbm else x for k, x in enumerate(ins)])


def swap(x, axis):
    return lax.ppermute(x, axis, [(k, k ^ 1) for k in range(lax.axis_size(axis))])


def far_swap(x, axis):
    n, m = lax.axis_size("row"), lax.axis_size("col")

    def partner(r, c):
        if axis == "col":
            return r, (c + 1) % m if c % 2 else (c - 1) % m
        if r in (0, n - 1):
            return r, c ^ 1
        return (r + 1 if r % 2 else r - 1), c

    pairs = []
    for r in range(n):
        for c in range(m):
            to = partner(r, c)
            pairs.append((r * m + c, to[0] * m + to[1]))
    return lax.ppermute(x, ("row", "col"), pairs)


def swap_both(a, b, axis):
    b = far_swap(b, axis)
    a = swap(a, axis)
    return a, b


def shift(x, axis, by):
    n = lax.axis_size(axis)
    return lax.ppermute(x, axis, [(k, (k + by) % n) for k in range(n)])


def exchange_sums(part):
    both = part + swap(part, "col")
    up = shift(both[:, 2 * REACH :], "col", 2)
    down = shift(both[:, : 2 * REACH], "col", -2)
    return both, up, down


EXT_SHAPE = shape(WIDE * EXT, 128)
GRID = shape(WIDE, ROWS, 128)
BAND = shape(2, WIDE, 8, 128)
SEG_ROWS = pltpu.VMEM((SEG, 128), F32)
SUMS = pltpu.VMEM((16, SEG), F32)
OTHER = pltpu.VMEM((WIDE * EXT, 128), F32)
WORK = pltpu.VMEM((2, WIDE, 32, 128), F32)
SPARE = pltpu.VMEM((2, WIDE, 8, 128), F32)
TURN = pltpu.VMEM((128, ROWS), F32)
SMALL = pltpu.SMEM((8, 128), I32)


def sems(n):
    return pltpu.SemaphoreType.DMA((n,))


def body(head0, recharge, storage, seg_block, seg_mask, seg_cond, seg_reach, bed, sec0, net, infl):
    part, oh, weight, head, index8, rech = call(
        prep,
        (shape(8, FRAME), shape(SEG, LOCAL, dtype=BF16), shape(SEG, 128), EXT_SHAPE, shape(8, 128, dtype=I32), shape(ROWS, COLS)),
        (
            head0,
            seg_block.reshape(8, 128),
            seg_reach.reshape(8, 128),
            seg_mask,
            seg_cond,
            bed.reshape(2, 128),
            sec0.reshape(2, 128),
            net.reshape(2, 128),
            infl,
            recharge,
        ),
        scratch=[
            SEG_ROWS,
            SUMS,
            pltpu.VMEM((8, 128), I32),
            pltpu.VMEM((8, 128), I32),
            pltpu.VMEM((SEG, 128), I32),
            SEG_ROWS,
            pltpu.VMEM((2, 128), F32),
            pltpu.VMEM((2, 128), F32),
            pltpu.VMEM((2, 128), I32),
            pltpu.SMEM((NETS,), F32),
            SMALL,
            sems(18),
        ],
        hbm=range(10),
    )
    own, up, down = exchange_sums(part)
    (onehot,) = call(one_hot, (shape(TILES * ROWS, SEG, dtype=BF16),), (index8,))
    inv, supply = call(
        fields, (GRID, shape(TILES, ROWS, 128)), (head, rech, storage, weight, onehot)
    )
    strip = shape(16, ROWS)
    pa, pb = call(functools.partial(columns, True), (strip, strip), (head, inv))
    mixed_shape = shape(SEG, 256, dtype=BF16)
    frame, mixed, rhs, ma, mb = call(
        functools.partial(section_kernel, True),
        (shape(8, FRAME), mixed_shape, GRID, strip, strip),
        (own, up, down, oh, onehot, weight, supply, pa, pb),
    )
    ca, cb = swap_both(ma, mb, "col")
    (rhs,) = call(inner_source, (GRID,), (onehot, mixed, supply, rhs), aliases={3: 0})
    rows = shape(96, 128)
    head, rhs, inv, sa, sb, band = call(
        functools.partial(place_columns, True),
        (EXT_SHAPE, GRID, GRID, rows, rows, BAND),
        (ca, cb, head, rhs, inv),
        scratch=[TURN],
        aliases={2: 0, 3: 1, 4: 2},
    )
    ra, rb = swap_both(sa, sb, "row")
    (head,) = call(inner_relax, (EXT_SHAPE,), (head, rhs, inv), scratch=[OTHER], aliases={0: 0})
    head, rim, part = call(
        finish_first,
        (EXT_SHAPE, BAND, shape(1, FRAME)),
        (ra, rb, band, head, rhs, inv, index8, weight, oh),
        scratch=[WORK, WORK, SEG_ROWS, SUMS, SPARE, SMALL, pltpu.SemaphoreType.DMA],
        aliases={3: 0},
    )
    own, up, down = exchange_sums(part)
    strip = shape(8, ROWS)
    pa, pb = call(functools.partial(columns, False), (strip, strip), (head,))
    reaches, mixed, rhs, ma, mb = call(
        functools.partial(section_kernel, False),
        (shape(1, FRAME), mixed_shape, GRID, strip, strip),
        (own, up, down, frame, oh, onehot, weight, supply, pa, pb),
    )
    ca, cb = swap_both(ma, mb, "col")
    (rhs,) = call(inner_source, (GRID,), (onehot, mixed, supply, rhs), aliases={3: 0})
    rows = shape(64, 128)
    head, rhs, sa, sb, band = call(
        functools.partial(place_columns, False),
        (EXT_SHAPE, GRID, rows, rows, BAND),
        (ca, cb, head, rhs),
        scratch=[TURN],
        aliases={2: 0, 3: 1},
    )
    ra, rb = swap_both(sa, sb, "row")
    (head,) = call(inner_relax, (EXT_SHAPE,), (head, rhs, inv), scratch=[OTHER], aliases={0: 0})
    out, section = call(
        finish_last,
        (shape(ROWS, COLS), shape(2, 128)),
        (ra, rb, band, head, rhs, inv, rim, reaches),
        scratch=[WORK, WORK, SPARE, pltpu.VMEM((2, 8, COLS), F32), pltpu.VMEM((2, 128), F32), sems(3 + TILES)],
        hbm_out=(0, 1),
    )
    return out, section.reshape(REACH)


def solution(mesh):
    placed = (
        P("row", "col"),
        P("row", "col"),
        P("row", "col"),
        P(("row", "col")),
        P(("row", "col"), None),
        P(("row", "col"), None),
        P(("row", "col")),
        P(("row", "col")),
        P(("row", "col")),
        P(("row", "col")),
        P(),
    )
    return jax.shard_map(
        body,
        mesh=mesh,
        in_specs=placed,
        out_specs=(P("row", "col"), P(("row", "col"))),
        check_vma=False,
    )
```
